32 devices in a mesh: data: 4 (over z), cp: 8 (over y, x, core).
Axes of the slice: x: 2, y: 2, z: 4, core: 2. Of those that a mesh axis runs over, the one named last changes fastest.
Arguments:
- q: bfloat16 [32768, 4, 128], P(('data', 'cp')), parts along dimension 0
- k: bfloat16 [32768, 4, 128], P(('data', 'cp')), parts along dimension 0
- v: bfloat16 [32768, 4, 128], P(('data', 'cp')), parts along dimension 0
- o: bfloat16 [32768, 4, 128], P(('data', 'cp')), parts along dimension 0
- dout: bfloat16 [32768, 4, 128], P(('data', 'cp')), parts along dimension 0
- lse: float32 [4, 32768], P(None, ('data', 'cp')), parts along dimension 1
Outputs:
- output 1: bfloat16 [32768, 4, 128], P(('data', 'cp')), parts along dimension 0
- output 2: bfloat16 [32768, 4, 128], P(('data', 'cp')), parts along dimension 0
- output 3: bfloat16 [32768, 4, 128], P(('data', 'cp')), parts along dimension 0
There are 4 independent parts. The reference program is written for one: setup_inputs(seed, part) draws one part's arguments, and reference() takes and returns one part's arrays. A program takes and returns all parts, laid end to end along the dimension named above; each array names one.
All inputs are finite; a program needn't handle non-finite values.
Results may differ from the reference program's by a relative error of at most 0.001.
Values are sent between devices in bfloat16 or wider.
A program may use at most 1 GiB of HBM per device.

```python
import math
import jax
import jax.numpy as jnp
from jax import lax

C = 1024
CP = 8
HEADS = 4
HEAD = 128
QB = 128

T = C * CP
SCALE = 1.0 / math.sqrt(HEAD)


def positions():
    r = jnp.arange(T, dtype=jnp.int32)
    return (r % C) * CP + r // C


def _head_forward(q, k, v, pos):
    def blk(b):
        qb = lax.dynamic_slice_in_dim(q, b * QB, QB)
        pb = lax.dynamic_slice_in_dim(pos, b * QB, QB)
        s = jnp.dot(qb, k.T, preferred_element_type=jnp.float32) * SCALE
        s = jnp.where(pos[None, :] <= pb[:, None], s, -jnp.inf)
        mx = jnp.max(s, axis=1, keepdims=True)
        e = jnp.exp(s - mx)
        l = jnp.sum(e, axis=1, keepdims=True)
        o = jnp.dot((e / l).astype(jnp.bfloat16), v, preferred_element_type=jnp.float32)
        return o.astype(jnp.bfloat16), (mx + jnp.log(l))[:, 0]
    o, lse = lax.map(blk, jnp.arange(T // QB))
    return o.reshape(T, HEAD), lse.reshape(T)


def _forward(q, k, v):
    pos = positions()
    o, lse = lax.map(lambda a: _head_forward(a[0], a[1], a[2], pos),
                     (q.transpose(1, 0, 2), k.transpose(1, 0, 2), v.transpose(1, 0, 2)))
    return o.transpose(1, 0, 2), lse


def setup_inputs(seed: int = 0, part: int = 0) -> dict:
    key = jax.random.fold_in(jax.random.PRNGKey(seed), part)
    kq, kk, km, kv, kd = jax.random.split(key, 5)
    shape = (T, HEADS, HEAD)
    q = jax.random.normal(kq, shape, jnp.float32).astype(jnp.bfloat16)
    k = jax.random.normal(kk, shape, jnp.float32).astype(jnp.bfloat16)
    mu = jax.random.normal(km, (1, HEADS, HEAD), jnp.float32)
    v = (0.8 * mu + 0.6 * jax.random.normal(kv, shape, jnp.float32)).astype(jnp.bfloat16)
    o, lse = _forward(q, k, v)
    dout = (0.8 * o.astype(jnp.float32) + 0.6 * jax.random.normal(kd, shape, jnp.float32)).astype(jnp.bfloat16)
    return {'q': q, 'k': k, 'v': v, 'o': o, 'dout': dout, 'lse': lse}


def reference(q, k, v, o, dout, lse):
    pos = positions()
    dd = jnp.sum(dout.astype(jnp.float32) * o.astype(jnp.float32), axis=-1)

    def head(a):
        qh, kh, vh, doh, lh, dh = a

        def step(carry, b):
            dk, dv = carry
            qb = lax.dynamic_slice_in_dim(qh, b * QB, QB)
            dob = lax.dynamic_slice_in_dim(doh, b * QB, QB)
            lb = lax.dynamic_slice_in_dim(lh, b * QB, QB)
            db = lax.dynamic_slice_in_dim(dh, b * QB, QB)
            pb = lax.dynamic_slice_in_dim(pos, b * QB, QB)
            s = jnp.dot(qb, kh.T, preferred_element_type=jnp.float32) * SCALE
            mask = pos[None, :] <= pb[:, None]
            p = jnp.where(mask, jnp.exp(s - lb[:, None]), 0.0)
            dv = dv + jnp.dot(p.astype(jnp.bfloat16).T, dob, preferred_element_type=jnp.float32)
            dp = jnp.dot(dob, vh.T, preferred_element_type=jnp.float32)
            ds = (p * (dp - db[:, None])).astype(jnp.bfloat16)
            dqb = jnp.dot(ds, kh, preferred_element_type=jnp.float32) * SCALE
            dk = dk + jnp.dot(ds.T, qb, preferred_element_type=jnp.float32) * SCALE
            return (dk, dv), dqb

        z = jnp.zeros((T, HEAD), jnp.float32)
        (dk, dv), dq = lax.scan(step, (z, z), jnp.arange(T // QB))
        return dq.reshape(T, HEAD), dk, dv

    dq, dk, dv = lax.map(head, (q.transpose(1, 0, 2), k.transpose(1, 0, 2), v.transpose(1, 0, 2),
                                dout.transpose(1, 0, 2), lse, dd.T))
    return (dq.transpose(1, 0, 2).astype(jnp.bfloat16),
            dk.transpose(1, 0, 2).astype(jnp.bfloat16),
            dv.transpose(1, 0, 2).astype(jnp.bfloat16))
```

```python
import functools
import math

import jax
import jax.numpy as jnp
from jax import lax
from jax.experimental import pallas as pl
from jax.experimental.pallas import tpu as pltpu
from jax.sharding import PartitionSpec as P

MESH = pl.DeviceIdType.MESH
F32 = jnp.float32
BF16 = jnp.bfloat16
ROWS = 128
LOG2E = math.log2(math.e)


def _dot(a, b, ca, cb):
    return lax.dot_general(a, b, (((ca,), (cb,)), ((), ())), preferred_element_type=F32)


def _kernel(nb, x, aux, out, rx, rs, axr, kt, dk, dv, dqt, dqp, okv, oq,
            in_s, in_r, in_l, fw_s, fw_r, ax_s, ax_r, ax_l, kv_s, kv_r, kv_l,
            qp_s, qp_r, oq_s, oq_r, oq_l):
    hd = x.shape[-1]
    tile = 4 * ROWS
    scale = hd ** -0.5
    me = lax.axis_index('cp')
    core = me % 2
    chip = me // 2
    cx, cy = chip % 2, chip // 2
    sib = chip * 2 + (1 - core)
    rel = [cy * 2 + (1 - cx), (1 - cy) * 2 + cx, 3 - chip]

    barrier = pltpu.get_barrier_semaphore()
    for t in range(1, 8):
        pl.semaphore_signal(barrier, inc=1, device_id={'cp': (me + t) % 8}, device_id_type=MESH)
    pl.semaphore_wait(barrier, 7)

    def remote(src, dst, ss, rsem, dev):
        return pltpu.make_async_remote_copy(src_ref=src, dst_ref=dst, send_sem=ss, recv_sem=rsem,
                                            device_id={'cp': dev}, device_id_type=MESH)

    def rows(b):
        return pl.ds(pl.multiple_of(b * ROWS, ROWS), ROWS)

    def aux_send(t):
        dev = (me + t) % 8
        return remote(aux.at[dev // 2], axr.at[core, chip], ax_s.at[t - 1], ax_r.at[t - 1], dev)

    def aux_recv(t):
        dev = (me + 8 - t) % 8
        return remote(aux.at[0], axr.at[dev % 2, dev // 2], ax_s.at[t - 1], ax_r.at[t - 1], dev)

    def in_send(b, d):
        return remote(x.at[:, rel[d], rows(b)], rx.at[b, chip], in_s.at[b, d], in_r.at[b, d], rel[d] * 2 + core)

    def in_recv(b, d):
        return remote(x.at[:, 0, rows(b)], rx.at[b, rel[d]], in_s.at[b, d], in_r.at[b, d], rel[d] * 2 + core)

    def in_local(b):
        return pltpu.make_async_copy(x.at[:, chip, rows(b)], rx.at[b, chip], in_l.at[b])

    def forward(b):
        return remote(rx.at[b, :, 0:2], rs.at[b], fw_s.at[b], fw_r.at[b], sib)

    def kv_send(b, d):
        return remote(okv.at[b, :, rel[d]], out.at[1:3, chip, rows(b)], kv_s.at[b, d], kv_r.at[b, d], rel[d] * 2 + core)

    def kv_recv(b, d):
        return remote(okv.at[b, :, rel[d]], out.at[1:3, rel[d], rows(b)], kv_s.at[b, d], kv_r.at[b, d], rel[d] * 2 + core)

    def kv_local(b):
        return pltpu.make_async_copy(okv.at[b, :, chip], out.at[1:3, chip, rows(b)], kv_l.at[b])

    def part_send(b):
        return remote(dqt.at[1, b], dqp.at[b], qp_s.at[b], qp_r.at[b], sib)

    def q_send(b, d):
        return remote(oq.at[b, rel[d]], out.at[0, chip, rows(b)], oq_s.at[b, d], oq_r.at[b, d], rel[d] * 2 + core)

    def q_recv(b, d):
        return remote(oq.at[b, rel[d]], out.at[0, rel[d], rows(b)], oq_s.at[b, d], oq_r.at[b, d], rel[d] * 2 + core)

    def q_local(b):
        return pltpu.make_async_copy(oq.at[b, chip], out.at[0, chip, rows(b)], oq_l.at[b])

    own_aux = pltpu.make_async_copy(aux.at[chip], axr.at[core, chip], ax_l.at[0])
    own_aux.start()
    for t in range(1, 8):
        aux_send(t).start()

    def issue(n, c):
        b = nb - 1 - n
        in_local(b).start()
        for d in (2, 0, 1):
            in_send(b, d).start()
        return c

    lax.fori_loop(0, nb, issue, 0)
    own_aux.wait()
    for t in range(1, 8):
        aux_recv(t).wait_recv()

    kidx = lax.broadcasted_iota(jnp.int32, (tile, 1), 0)
    qidx = lax.broadcasted_iota(jnp.int32, (1, tile), 1)
    kpos = (kidx % ROWS) * 8 + (kidx // ROWS) * 2 + core

    def pair(b, qb, other, diag, fresh=False):
        if other:
            q = rs[qb, :, 0].reshape(tile, hd)
            do = rs[qb, :, 1].reshape(tile, hd)
            par = 1 - core
        else:
            q = rx[qb, :, 0].reshape(tile, hd)
            do = rx[qb, :, 1].reshape(tile, hd)
            par = core
        k = rx[b, :, 2].reshape(tile, hd)
        v = rx[b, :, 3].reshape(tile, hd)
        lse = jnp.concatenate([axr[par, i, qb] for i in range(4)], axis=1)
        dd = jnp.concatenate([axr[par, i, qb + nb] for i in range(4)], axis=1)
        s = _dot(k, q, 1, 1)
        p = jnp.exp2(s * (scale * LOG2E) - lse)
        if diag:
            qpos = (qidx % ROWS) * 8 + (qidx // ROWS) * 2 + par
            p = jnp.where(kpos <= qpos, p, 0.0)
        dp = _dot(v, do, 1, 1)
        ds = (p * (dp - dd)).astype(BF16)
        gv = _dot(p.astype(BF16), do, 1, 0)
        gk = _dot(ds, q, 1, 0)
        gq = _dot(kt[...], ds, 1, 0)
        if fresh:
            dv[...] = gv
            dk[...] = gk
        else:
            dv[...] += gv
            dk[...] += gk
        if diag:
            dqt[int(other), qb] = gq
        else:
            dqt[int(other), qb] += gq

    def arrive(b):
        for d in range(3):
            in_recv(b, d).wait_recv()
        in_local(b).wait()
        forward(b).start()
        kt[...] = rx[b, :, 2].reshape(tile, hd).astype(F32).T.astype(BF16)

    def emit_kv(b):
        okv[b, 0] = (dk[...] * scale).astype(BF16).reshape(4, ROWS, hd)
        okv[b, 1] = dv[...].astype(BF16).reshape(4, ROWS, hd)
        kv_local(b).start()
        for d in (2, 0, 1):
            kv_send(b, d).start()

    def step(n, c):
        b = nb - 1 - n
        arrive(b)
        pair(b, b, False, True, fresh=True)

        def own(i, c):
            pair(b, i, False, False)
            return c

        lax.fori_loop(b + 1, nb, own, 0)
        forward(b).wait_recv()
        pair(b, b, True, True)

        def oth(i, c):
            pair(b, i, True, False)
            return c

        lax.fori_loop(b + 1, nb, oth, 0)
        emit_kv(b)
        return c

    lax.fori_loop(0, nb - 1, step, 0)

    arrive(0)
    dv[...] = jnp.zeros_like(dv)
    dk[...] = jnp.zeros_like(dk)

    def finish(i):
        part_send(i).wait_recv()
        g = (dqt[0, i] + dqp[i]) * scale
        oq[i] = g.T.astype(BF16).reshape(4, ROWS, hd)
        q_local(i).start()
        for d in (2, 0, 1):
            q_send(i, d).start()

    def last_oth(n, c):
        i = nb - 1 - n
        pair(0, i, True, False)
        part_send(i).start()
        return c

    lax.fori_loop(0, nb - 1, last_oth, 0)
    forward(0).wait_recv()
    pair(0, 0, True, True)
    part_send(0).start()

    def last_own(n, c):
        i = nb - 1 - n
        pair(0, i, False, False)
        finish(i)
        return c

    lax.fori_loop(0, nb - 1, last_own, 0)
    pair(0, 0, False, True)
    emit_kv(0)
    finish(0)

    for t in range(1, 8):
        aux_send(t).wait_send()

    def drain(b, c):
        for d in range(3):
            in_send(b, d).wait_send()
            kv_send(b, d).wait_send()
            kv_recv(b, d).wait_recv()
            q_send(b, d).wait_send()
            q_recv(b, d).wait_recv()
        forward(b).wait_send()
        part_send(b).wait_send()
        kv_local(b).wait()
        q_local(b).wait()
        return c

    lax.fori_loop(0, nb, drain, 0)


def solution(mesh):
    rows = P(('data', 'cp'))
    cols = P(None, ('data', 'cp'))

    def local(q, k, v, o, dout, lse):
        c, h, d = q.shape
        nb = c // ROWS
        dd = jnp.einsum('qhd,qhd->hq', dout, o, preferred_element_type=F32)
        x = jnp.stack([a.transpose(1, 0, 2) for a in (q, dout, k, v)])
        aux = jnp.concatenate([(lse * LOG2E).reshape(h, nb, 1, ROWS), dd.reshape(h, nb, 1, ROWS)], axis=1)
        dma = pltpu.SemaphoreType.DMA
        out = pl.pallas_call(
            functools.partial(_kernel, nb),
            out_shape=jax.ShapeDtypeStruct((3, h, c, d), BF16),
            in_specs=[pl.BlockSpec(memory_space=pl.ANY)] * 2,
            out_specs=pl.BlockSpec(memory_space=pl.ANY),
            scratch_shapes=[
                pltpu.VMEM((nb, 4, 4, ROWS, d), BF16),
                pltpu.VMEM((nb, 4, 2, ROWS, d), BF16),
                pltpu.VMEM((2, 4, 2 * nb, 1, ROWS), F32),
                pltpu.VMEM((d, 4 * ROWS), BF16),
                pltpu.VMEM((4 * ROWS, d), F32),
                pltpu.VMEM((4 * ROWS, d), F32),
                pltpu.VMEM((2, nb, d, 4 * ROWS), F32),
                pltpu.VMEM((nb, d, 4 * ROWS), F32),
                pltpu.VMEM((nb, 2, 4, ROWS, d), BF16),
                pltpu.VMEM((nb, 4, ROWS, d), BF16),
                dma((nb, 3)), dma((nb, 3)), dma((nb,)),
                dma((nb,)), dma((nb,)),
                dma((7,)), dma((7,)), dma((1,)),
                dma((nb, 3)), dma((nb, 3)), dma((nb,)),
                dma((nb,)), dma((nb,)),
                dma((nb, 3)), dma((nb, 3)), dma((nb,)),
            ],
            compiler_params=pltpu.CompilerParams(
                collective_id=0, has_side_effects=True, vmem_limit_bytes=60 << 20),
            name='attn_bwd',
        )(x, aux)
        return tuple(out[i].transpose(1, 0, 2) for i in range(3))

    return jax.shard_map(local, mesh=mesh, in_specs=(rows, rows, rows, rows, rows, cols),
                         out_specs=(rows, rows, rows), check_vma=False)
```

```python
import functools
import math

import jax
import jax.numpy as jnp
from jax import lax
from jax.experimental import pallas as pl
from jax.experimental.pallas import tpu as pltpu
from jax.sharding import PartitionSpec as P

MESH = pl.DeviceIdType.MESH
F32 = jnp.float32
BF16 = jnp.bfloat16
ROWS = 128
VMEM_LIMIT = 52 << 20
LOG2E = math.log2(math.e)


def _dot(a, b, ca, cb):
    return lax.dot_general(a, b, (((ca,), (cb,)), ((), ())), preferred_element_type=F32)


def _kernel(nb, q_in, do_in, k_in, v_in, o_in, lse_in, dq_out, dk_out, dv_out,
            raw, lsev, xs, auxs, rx, rs, axr, kt, dk, dv, dqt, dqp, okv, oq, orx, ost,
            raw_l, lse_l, in_s, in_r, fw_s, fw_r, ax_s, ax_r, fa_s, fa_r, kv_s, kv_r,
            qp_s, qp_r, oq_s, oq_r, out_l):
    hd = q_in.shape[-1]
    tile = 4 * ROWS
    scale = hd ** -0.5
    me = lax.axis_index('cp')
    core = me % 2
    chip = me // 2
    cx, cy = chip % 2, chip // 2
    sib = chip * 2 + (1 - core)
    rel = [cy * 2 + (1 - cx), (1 - cy) * 2 + cx, 3 - chip]

    def remote(src, dst, ss, rsem, dev):
        return pltpu.make_async_remote_copy(src_ref=src, dst_ref=dst, send_sem=ss, recv_sem=rsem,
                                            device_id={'cp': dev}, device_id_type=MESH)

    def rows(b):
        return pl.ds(pl.multiple_of(b * ROWS, ROWS), ROWS)

    def raw_copy(i, b):
        src = (q_in, do_in, k_in, v_in, o_in)[i]
        return pltpu.make_async_copy(src.at[rows(b)], raw.at[b, i], raw_l.at[b, i])

    def in_send(b, d):
        return remote(xs.at[b, rel[d]], rx.at[b, chip], in_s.at[b, d], in_r.at[b, d], rel[d] * 2 + core)

    def in_recv(b, d):
        return remote(xs.at[b, rel[d]], rx.at[b, rel[d]], in_s.at[b, d], in_r.at[b, d], rel[d] * 2 + core)

    def aux_send(b, d):
        return remote(auxs.at[b, rel[d]], axr.at[b, core, chip], ax_s.at[b, d], ax_r.at[b, d], rel[d] * 2 + core)

    def aux_recv(b, d):
        return remote(auxs.at[b, rel[d]], axr.at[b, core, rel[d]], ax_s.at[b, d], ax_r.at[b, d], rel[d] * 2 + core)

    def forward(b):
        return remote(rx.at[b, :, 0:2], rs.at[b], fw_s.at[b], fw_r.at[b], sib)

    def aux_forward(b):
        return remote(axr.at[b, core], axr.at[b, core], fa_s.at[b], fa_r.at[b], sib)

    def aux_forwarded(b):
        return remote(axr.at[b, core], axr.at[b, 1 - core], fa_s.at[b], fa_r.at[b], sib)

    def kv_send(b, d):
        return remote(okv.at[b, :, rel[d]], orx.at[b, 1:3, chip], kv_s.at[b, d], kv_r.at[b, d], rel[d] * 2 + core)

    def kv_recv(b, d):
        return remote(okv.at[b, :, rel[d]], orx.at[b, 1:3, rel[d]], kv_s.at[b, d], kv_r.at[b, d], rel[d] * 2 + core)

    def part_send(b):
        return remote(dqt.at[1, b], dqp.at[b], qp_s.at[b], qp_r.at[b], sib)

    def q_send(b, d):
        return remote(oq.at[b, rel[d]], orx.at[b, 0, chip], oq_s.at[b, d], oq_r.at[b, d], rel[d] * 2 + core)

    def q_recv(b, d):
        return remote(oq.at[b, rel[d]], orx.at[b, 0, rel[d]], oq_s.at[b, d], oq_r.at[b, d], rel[d] * 2 + core)

    def out_copy(a, b):
        return pltpu.make_async_copy(ost.at[b, a], (dq_out, dk_out, dv_out)[a].at[rows(b)], out_l.at[b, a])

    lse_copy = pltpu.make_async_copy(lse_in, lsev, lse_l.at[0])
    lse_copy.start()

    def load(n, c):
        for i in range(5):
            raw_copy(i, nb - 1 - n).start()
        return c

    lax.fori_loop(0, nb, load, 0)

    barrier = pltpu.get_barrier_semaphore()
    peers = [r * 2 + core for r in rel] + [sib]
    for p in peers:
        pl.semaphore_signal(barrier, inc=1, device_id={'cp': p}, device_id_type=MESH)
    lse_copy.wait()

    eye = (lax.broadcasted_iota(jnp.int32, (ROWS, ROWS), 0)
           == lax.broadcasted_iota(jnp.int32, (ROWS, ROWS), 1))

    def prepare(b):
        for i in range(5):
            raw_copy(i, b).wait()
        for i in range(4):
            xs[b, :, i] = jnp.swapaxes(raw[b, i], 0, 1)
        oh = jnp.swapaxes(raw[b, 4], 0, 1)
        lse = lsev[:, rows(b)] * LOG2E
        for h in range(4):
            g = _dot(xs[b, h, 1], oh[h], 1, 1)
            auxs[b, h, 0] = lse[h:h + 1]
            auxs[b, h, 1] = jnp.sum(jnp.where(eye, g, 0.0), axis=0, keepdims=True)

    def dispatch(b):
        for d in (2, 0, 1):
            aux_send(b, d).start()
            in_send(b, d).start()
        rx[b, chip] = xs[b, chip]
        axr[b, core, chip] = auxs[b, chip]

    prepare(nb - 1)
    pl.semaphore_wait(barrier, 4)
    dispatch(nb - 1)

    def issue(n, c):
        b = nb - 1 - n
        prepare(b)
        dispatch(b)
        return c

    lax.fori_loop(1, nb, issue, 0)

    kidx = lax.broadcasted_iota(jnp.int32, (tile, 1), 0)
    qidx = lax.broadcasted_iota(jnp.int32, (1, tile), 1)
    kpos = (kidx % ROWS) * 8 + (kidx // ROWS) * 2 + core

    def pair(b, qb, other, diag, fresh=False):
        if other:
            q = rs[qb, :, 0].reshape(tile, hd)
            do = rs[qb, :, 1].reshape(tile, hd)
            par = 1 - core
        else:
            q = rx[qb, :, 0].reshape(tile, hd)
            do = rx[qb, :, 1].reshape(tile, hd)
            par = core
        k = rx[b, :, 2].reshape(tile, hd)
        v = rx[b, :, 3].reshape(tile, hd)
        lse = jnp.concatenate([axr[qb, par, i, 0] for i in range(4)], axis=1)
        dd = jnp.concatenate([axr[qb, par, i, 1] for i in range(4)], axis=1)
        s = _dot(k, q, 1, 1)
        p = jnp.exp2(s * (scale * LOG2E) - lse)
        if diag:
            qpos = (qidx % ROWS) * 8 + (qidx // ROWS) * 2 + par
            p = jnp.where(kpos <= qpos, p, 0.0)
        dp = _dot(v, do, 1, 1)
        ds = (p * (dp - dd)).astype(BF16)
        gv = _dot(p.astype(BF16), do, 1, 0)
        gk = _dot(ds, q, 1, 0)
        gq = _dot(kt[...], ds, 1, 0)
        if fresh:
            dv[...] = gv
            dk[...] = gk
        else:
            dv[...] += gv
            dk[...] += gk
        if diag:
            dqt[int(other), qb] = gq
        else:
            dqt[int(other), qb] += gq

    def arrive(b):
        for d in range(3):
            in_recv(b, d).wait_recv()
            aux_recv(b, d).wait_recv()
        forward(b).start()
        aux_forward(b).start()
        kt[...] = rx[b, :, 2].reshape(tile, hd).astype(F32).T.astype(BF16)

    def emit_kv(b):
        okv[b, 0] = (dk[...] * scale).astype(BF16).reshape(4, ROWS, hd)
        okv[b, 1] = dv[...].astype(BF16).reshape(4, ROWS, hd)
        for d in (2, 0, 1):
            kv_send(b, d).start()
        orx[b, 1:3, chip] = okv[b, :, chip]

    def step(n, c):
        b = nb - 1 - n
        arrive(b)
        pair(b, b, False, True, fresh=True)

        def own(i, c):
            pair(b, i, False, False)
            return c

        lax.fori_loop(b + 1, nb, own, 0)
        forward(b).wait_recv()
        aux_forwarded(b).wait_recv()
        pair(b, b, True, True)

        def oth(i, c):
            pair(b, i, True, False)
            return c

        lax.fori_loop(b + 1, nb, oth, 0)
        emit_kv(b)
        return c

    lax.fori_loop(0, nb - 1, step, 0)

    arrive(0)
    dv[...] = jnp.zeros_like(dv)
    dk[...] = jnp.zeros_like(dk)

    def finish(i):
        part_send(i).wait_recv()
        g = (dqt[0, i] + dqp[i]) * scale
        oq[i] = g.T.astype(BF16).reshape(4, ROWS, hd)
        for d in (2, 0, 1):
            q_send(i, d).start()
        orx[i, 0, chip] = oq[i, chip]

    def last_oth(n, c):
        i = nb - 1 - n
        pair(0, i, True, False)
        part_send(i).start()
        return c

    lax.fori_loop(0, nb - 1, last_oth, 0)
    forward(0).wait_recv()
    aux_forwarded(0).wait_recv()
    pair(0, 0, True, True)
    part_send(0).start()

    def last_own(n, c):
        i = nb - 1 - n
        pair(0, i, False, False)
        finish(i)
        return c

    lax.fori_loop(0, nb - 1, last_own, 0)
    pair(0, 0, False, True)
    emit_kv(0)
    finish(0)

    def put(a, b):
        ost[b, a] = jnp.swapaxes(orx[b, a], 0, 1)
        out_copy(a, b).start()

    def out_kv(b):
        for d in range(3):
            kv_recv(b, d).wait_recv()
        put(1, b)
        put(2, b)

    def out_q(b):
        for d in range(3):
            q_recv(b, d).wait_recv()
        put(0, b)

    def drain_kv(n, c):
        out_kv(nb - 1 - n)
        return c

    def drain_q(n, c):
        out_q(nb - 1 - n)
        return c

    lax.fori_loop(0, nb - 1, drain_kv, 0)
    lax.fori_loop(0, nb - 1, drain_q, 0)
    out_kv(0)
    out_q(0)

    def drain(b, c):
        for d in range(3):
            in_send(b, d).wait_send()
            aux_send(b, d).wait_send()
            kv_send(b, d).wait_send()
            q_send(b, d).wait_send()
        forward(b).wait_send()
        aux_forward(b).wait_send()
        part_send(b).wait_send()
        for a in range(3):
            out_copy(a, b).wait()
        return c

    lax.fori_loop(0, nb, drain, 0)


def solution(mesh):
    rows = P(('data', 'cp'))
    cols = P(None, ('data', 'cp'))

    def local(q, k, v, o, dout, lse):
        c, h, d = q.shape
        nb = c // ROWS
        vm, dma = pltpu.VMEM, pltpu.SemaphoreType.DMA
        any_ = pl.BlockSpec(memory_space=pl.ANY)
        return pl.pallas_call(
            functools.partial(_kernel, nb),
            out_shape=[jax.ShapeDtypeStruct((c, h, d), BF16)] * 3,
            in_specs=[any_] * 6,
            out_specs=[any_] * 3,
            scratch_shapes=[
                vm((nb, 5, ROWS, h, d), BF16),
                vm((h, c), F32),
                vm((nb, h, 4, ROWS, d), BF16),
                vm((nb, h, 2, 1, ROWS), F32),
                vm((nb, 4, 4, ROWS, d), BF16),
                vm((nb, 4, 2, ROWS, d), BF16),
                vm((nb, 2, 4, 2, 1, ROWS), F32),
                vm((d, 4 * ROWS), BF16),
                vm((4 * ROWS, d), F32),
                vm((4 * ROWS, d), F32),
                vm((2, nb, d, 4 * ROWS), F32),
                vm((nb, d, 4 * ROWS), F32),
                vm((nb, 2, 4, ROWS, d), BF16),
                vm((nb, 4, ROWS, d), BF16),
                vm((nb, 3, h, ROWS, d), BF16),
                vm((nb, 3, ROWS, h, d), BF16),
                dma((nb, 5)), dma((1,)),
                dma((nb, 3)), dma((nb, 3)),
                dma((nb,)), dma((nb,)),
                dma((nb, 3)), dma((nb, 3)),
                dma((nb,)), dma((nb,)),
                dma((nb, 3)), dma((nb, 3)),
                dma((nb,)), dma((nb,)),
                dma((nb, 3)), dma((nb, 3)),
                dma((nb, 3)),
            ],
            compiler_params=pltpu.CompilerParams(
                collective_id=0, has_side_effects=True, vmem_limit_bytes=VMEM_LIMIT),
            name='attn_bwd',
        )(q, dout, k, v, o, lse)

    return jax.shard_map(local, mesh=mesh, in_specs=(rows, rows, rows, rows, rows, cols),
                         out_specs=(rows, rows, rows), check_vma=False)
```

```python
import functools
import math

import jax
import jax.numpy as jnp
from jax import lax
from jax.experimental import pallas as pl
from jax.experimental.pallas import tpu as pltpu
from jax.sharding import PartitionSpec as P

MESH = pl.DeviceIdType.MESH
F32 = jnp.float32
BF16 = jnp.bfloat16
ROWS = 128
VMEM_LIMIT = 50 << 20
LOG2E = math.log2(math.e)


def _dot(a, b, ca, cb):
    return lax.dot_general(a, b, (((ca,), (cb,)), ((), ())), preferred_element_type=F32)


def _kernel(nb, q_in, do_in, k_in, v_in, o_in, lse_in, dq_out, dk_out, dv_out,
            raw, lsev, xs, auxs, rx, rs, axr, kt, dk, dv, dqt, dqp, okv, oq, orx,
            raw_l, lse_l, in_s, in_r, fw_s, fw_r, ax_s, ax_r, fa_s, fa_r, kv_s, kv_r,
            qp_s, qp_r, oq_s, oq_r):
    hd = q_in.shape[-1]
    tile = 4 * ROWS
    scale = hd ** -0.5
    me = lax.axis_index('cp')
    core = me % 2
    chip = me // 2
    cx, cy = chip % 2, chip // 2
    sib = chip * 2 + (1 - core)
    rel = [cy * 2 + (1 - cx), (1 - cy) * 2 + cx, 3 - chip]

    def remote(src, dst, ss, rsem, dev):
        return pltpu.make_async_remote_copy(src_ref=src, dst_ref=dst, send_sem=ss, recv_sem=rsem,
                                            device_id={'cp': dev}, device_id_type=MESH)

    def rows(b):
        return pl.ds(pl.multiple_of(b * ROWS, ROWS), ROWS)

    def raw_copy(i, b):
        src = (q_in, do_in, k_in, v_in, o_in)[i]
        return pltpu.make_async_copy(src.at[rows(b)], raw.at[b, i], raw_l.at[b, i])

    def in_send(b, d):
        return remote(xs.at[b, rel[d]], rx.at[b, chip], in_s.at[b, d], in_r.at[b, d], rel[d] * 2 + core)

    def in_recv(b, d):
        return remote(xs.at[b, rel[d]], rx.at[b, rel[d]], in_s.at[b, d], in_r.at[b, d], rel[d] * 2 + core)

    def aux_send(b, d):
        return remote(auxs.at[b, rel[d]], axr.at[b, core, chip], ax_s.at[b, d], ax_r.at[b, d], rel[d] * 2 + core)

    def aux_recv(b, d):
        return remote(auxs.at[b, rel[d]], axr.at[b, core, rel[d]], ax_s.at[b, d], ax_r.at[b, d], rel[d] * 2 + core)

    def forward(b):
        return remote(rx.at[b, :, 0:2], rs.at[b], fw_s.at[b], fw_r.at[b], sib)

    def aux_forward(b):
        return remote(axr.at[b, core], axr.at[b, core], fa_s.at[b], fa_r.at[b], sib)

    def aux_forwarded(b):
        return remote(axr.at[b, core], axr.at[b, 1 - core], fa_s.at[b], fa_r.at[b], sib)

    def kv_send(b, d):
        return remote(okv.at[b, :, rel[d]], orx.at[b, 1:3, chip], kv_s.at[b, d], kv_r.at[b, d], rel[d] * 2 + core)

    def kv_recv(b, d):
        return remote(okv.at[b, :, rel[d]], orx.at[b, 1:3, rel[d]], kv_s.at[b, d], kv_r.at[b, d], rel[d] * 2 + core)

    def part_send(b):
        return remote(dqt.at[1, b], dqp.at[b], qp_s.at[b], qp_r.at[b], sib)

    def q_send(b, d):
        return remote(oq.at[b, rel[d]], orx.at[b, 0, chip], oq_s.at[b, d], oq_r.at[b, d], rel[d] * 2 + core)

    def q_recv(b, d):
        return remote(oq.at[b, rel[d]], orx.at[b, 0, rel[d]], oq_s.at[b, d], oq_r.at[b, d], rel[d] * 2 + core)

    lse_copy = pltpu.make_async_copy(lse_in, lsev, lse_l.at[0])
    lse_copy.start()

    def load(n, c):
        for i in range(5):
            raw_copy(i, nb - 1 - n).start()
        return c

    lax.fori_loop(0, nb, load, 0)

    barrier = pltpu.get_barrier_semaphore()
    peers = [r * 2 + core for r in rel] + [sib]
    for p in peers:
        pl.semaphore_signal(barrier, inc=1, device_id={'cp': p}, device_id_type=MESH)
    lse_copy.wait()

    eye = (lax.broadcasted_iota(jnp.int32, (ROWS, ROWS), 0)
           == lax.broadcasted_iota(jnp.int32, (ROWS, ROWS), 1))

    def prepare(b):
        for i in range(5):
            raw_copy(i, b).wait()
        for i in range(4):
            xs[b, :, i] = jnp.swapaxes(raw[b, i], 0, 1)
        oh = jnp.swapaxes(raw[b, 4], 0, 1)
        lse = lsev[:, rows(b)] * LOG2E
        for h in range(4):
            g = _dot(xs[b, h, 1], oh[h], 1, 1)
            auxs[b, h, 0] = lse[h:h + 1]
            auxs[b, h, 1] = jnp.sum(jnp.where(eye, g, 0.0), axis=0, keepdims=True)

    def dispatch(b):
        for d in (2, 0, 1):
            aux_send(b, d).start()
            in_send(b, d).start()
        rx[b, chip] = xs[b, chip]
        axr[b, core, chip] = auxs[b, chip]

    prepare(nb - 1)
    pl.semaphore_wait(barrier, 4)
    dispatch(nb - 1)

    def issue(n, c):
        b = nb - 1 - n
        prepare(b)
        dispatch(b)
        return c

    lax.fori_loop(1, nb, issue, 0)

    kidx = lax.broadcasted_iota(jnp.int32, (tile, 1), 0)
    qidx = lax.broadcasted_iota(jnp.int32, (1, tile), 1)
    kpos = (kidx % ROWS) * 8 + (kidx // ROWS) * 2 + core

    def pair(b, qb, other, diag, fresh=False):
        if other:
            q = rs[qb, :, 0].reshape(tile, hd)
            do = rs[qb, :, 1].reshape(tile, hd)
            par = 1 - core
        else:
            q = rx[qb, :, 0].reshape(tile, hd)
            do = rx[qb, :, 1].reshape(tile, hd)
            par = core
        k = rx[b, :, 2].reshape(tile, hd)
        v = rx[b, :, 3].reshape(tile, hd)
        lse = jnp.concatenate([axr[qb, par, i, 0] for i in range(4)], axis=1)
        dd = jnp.concatenate([axr[qb, par, i, 1] for i in range(4)], axis=1)
        s = _dot(k, q, 1, 1)
        p = jnp.exp2(s * (scale * LOG2E) - lse)
        if diag:
            qpos = (qidx % ROWS) * 8 + (qidx // ROWS) * 2 + par
            p = jnp.where(kpos <= qpos, p, 0.0)
        dp = _dot(v, do, 1, 1)
        ds = (p * (dp - dd)).astype(BF16)
        gv = _dot(p.astype(BF16), do, 1, 0)
        gk = _dot(ds, q, 1, 0)
        gq = _dot(kt[...], ds, 1, 0)
        if fresh:
            dv[...] = gv
            dk[...] = gk
        else:
            dv[...] += gv
            dk[...] += gk
        if diag:
            dqt[int(other), qb] = gq
        else:
            dqt[int(other), qb] += gq

    def arrive(b):
        for d in range(3):
            in_recv(b, d).wait_recv()
            aux_recv(b, d).wait_recv()
        forward(b).start()
        aux_forward(b).start()

    def both(b, qb, diag):
        pair(b, qb, False, diag, fresh=diag)
        pair(b, qb, True, diag)

    def begin(b):
        kt[...] = rx[b, :, 2].reshape(tile, hd).astype(F32).T.astype(BF16)
        forward(b).wait_recv()
        aux_forwarded(b).wait_recv()

    def emit_kv(b):
        okv[b, 0] = (dk[...] * scale).astype(BF16).reshape(4, ROWS, hd)
        okv[b, 1] = dv[...].astype(BF16).reshape(4, ROWS, hd)
        for d in (2, 0, 1):
            kv_send(b, d).start()
        orx[b, 1:3, chip] = okv[b, :, chip]

    def step(n, c):
        b = nb - 1 - n
        begin(b)
        both(b, b, True)

        @pl.when(n == 0)
        def _():
            arrive(b - 1)

        def off(i, c):
            @pl.when(i == nb - 1)
            def _():
                arrive(b - 1)

            both(b, i, False)
            return c

        lax.fori_loop(b + 1, nb, off, 0)
        emit_kv(b)
        return c

    arrive(nb - 1)
    lax.fori_loop(0, nb - 1, step, 0)

    def finish(i):
        part_send(i).wait_recv()
        g = (dqt[0, i] + dqp[i]) * scale
        oq[i] = g.T.astype(BF16).reshape(4, ROWS, hd)
        for d in (2, 0, 1):
            q_send(i, d).start()
        orx[i, 0, chip] = oq[i, chip]

    begin(0)
    dv[...] = jnp.zeros_like(dv)
    dk[...] = jnp.zeros_like(dk)

    def last(n, c):
        i = nb - 1 - n
        both(0, i, False)
        part_send(i).start()

        @pl.when(n > 0)
        def _():
            finish(i + 1)

        return c

    lax.fori_loop(0, nb - 1, last, 0)
    pair(0, 0, True, True)
    part_send(0).start()
    pair(0, 0, False, True)
    emit_kv(0)
    finish(1)
    finish(0)

    def put(a, b):
        (dq_out, dk_out, dv_out)[a][rows(b)] = jnp.swapaxes(orx[b, a], 0, 1)

    def out_kv(b):
        for d in range(3):
            kv_recv(b, d).wait_recv()
        put(1, b)
        put(2, b)

    def out_q(b):
        for d in range(3):
            q_recv(b, d).wait_recv()
        put(0, b)

    def drain_kv(n, c):
        out_kv(nb - 1 - n)
        return c

    def drain_q(n, c):
        out_q(nb - 1 - n)
        return c

    lax.fori_loop(0, nb - 1, drain_kv, 0)
    lax.fori_loop(0, nb - 1, drain_q, 0)
    out_kv(0)
    out_q(0)

    def drain(b, c):
        for d in range(3):
            in_send(b, d).wait_send()
            aux_send(b, d).wait_send()
            kv_send(b, d).wait_send()
            q_send(b, d).wait_send()
        forward(b).wait_send()
        aux_forward(b).wait_send()
        part_send(b).wait_send()
        return c

    lax.fori_loop(0, nb, drain, 0)


def _store(a, b, c, x, y, z, sem):
    copies = [pltpu.make_async_copy(s, t, sem.at[i]) for i, (s, t) in enumerate(((a, x), (b, y), (c, z)))]
    for copy in copies:
        copy.start()
    for copy in copies:
        copy.wait()


def solution(mesh):
    rows = P(('data', 'cp'))
    cols = P(None, ('data', 'cp'))

    def local(q, k, v, o, dout, lse):
        c, h, d = q.shape
        nb = c // ROWS
        vm, dma = pltpu.VMEM, pltpu.SemaphoreType.DMA
        hbm = pl.BlockSpec(memory_space=pl.ANY)
        grads = pl.pallas_call(
            functools.partial(_kernel, nb),
            out_shape=[jax.ShapeDtypeStruct((c, h, d), BF16)] * 3,
            in_specs=[hbm] * 6,
            out_specs=[pl.BlockSpec(memory_space=pltpu.VMEM)] * 3,
            scratch_shapes=[
                vm((nb, 5, ROWS, h, d), BF16),
                vm((h, c), F32),
                vm((nb, h, 4, ROWS, d), BF16),
                vm((nb, h, 2, 1, ROWS), F32),
                vm((nb, 4, 4, ROWS, d), BF16),
                vm((nb, 4, 2, ROWS, d), BF16),
                vm((nb, 2, 4, 2, 1, ROWS), F32),
                vm((d, 4 * ROWS), BF16),
                vm((4 * ROWS, d), F32),
                vm((4 * ROWS, d), F32),
                vm((2, nb, d, 4 * ROWS), F32),
                vm((nb, d, 4 * ROWS), F32),
                vm((nb, 2, 4, ROWS, d), BF16),
                vm((nb, 4, ROWS, d), BF16),
                vm((nb, 3, h, ROWS, d), BF16),
                dma((nb, 5)), dma((1,)),
                dma((nb, 3)), dma((nb, 3)),
                dma((nb,)), dma((nb,)),
                dma((nb, 3)), dma((nb, 3)),
                dma((nb,)), dma((nb,)),
                dma((nb, 3)), dma((nb, 3)),
                dma((nb,)), dma((nb,)),
                dma((nb, 3)), dma((nb, 3)),
            ],
            compiler_params=pltpu.CompilerParams(
                collective_id=0, has_side_effects=True, vmem_limit_bytes=VMEM_LIMIT),
            name='attn_bwd',
        )(q, dout, k, v, o, lse)
        return pl.pallas_call(
            _store,
            out_shape=[jax.ShapeDtypeStruct((c, h, d), BF16)] * 3,
            in_specs=[pl.BlockSpec(memory_space=pltpu.VMEM)] * 3,
            out_specs=[hbm] * 3,
            scratch_shapes=[dma((3,))],
            compiler_params=pltpu.CompilerParams(vmem_limit_bytes=8 << 20),
            name='store',
        )(*grads)

    return jax.shard_map(local, mesh=mesh, in_specs=(rows, rows, rows, rows, rows, cols),
                         out_specs=(rows, rows, rows), check_vma=False)
```

```python
import functools
import math

import jax
import jax.numpy as jnp
from jax import lax
from jax.experimental import pallas as pl
from jax.experimental.pallas import tpu as pltpu
from jax.sharding import PartitionSpec as P

MESH = pl.DeviceIdType.MESH
F32 = jnp.float32
BF16 = jnp.bfloat16
ROWS = 128
VMEM_LIMIT = 50 << 20
LOG2E = math.log2(math.e)


def _dot(a, b, ca, cb):
    return lax.dot_general(a, b, (((ca,), (cb,)), ((), ())), preferred_element_type=F32)


def _kernel(nb, q_in, do_in, k_in, v_in, o_in, lse_in, dq_out, dk_out, dv_out,
            raw, lsev, xs, auxs, rx, rs, axr, kt, dk, dv, dqt, dqp, okv, oq, orx,
            raw_l, lse_l, in_s, in_r, fw_s, fw_r, ax_s, ax_r, fa_s, fa_r, kv_s, kv_r,
            qp_s, qp_r, oq_s, oq_r):
    hd = q_in.shape[-1]
    tile = 4 * ROWS
    scale = hd ** -0.5
    me = lax.axis_index('cp')
    core = me % 2
    chip = me // 2
    cx, cy = chip % 2, chip // 2
    sib = chip * 2 + (1 - core)
    rel = [cy * 2 + (1 - cx), (1 - cy) * 2 + cx, 3 - chip]

    def remote(src, dst, ss, rsem, dev):
        return pltpu.make_async_remote_copy(src_ref=src, dst_ref=dst, send_sem=ss, recv_sem=rsem,
                                            device_id={'cp': dev}, device_id_type=MESH)

    def rows(b):
        return pl.ds(pl.multiple_of(b * ROWS, ROWS), ROWS)

    def raw_copy(i, b):
        src = (q_in, do_in, k_in, v_in, o_in)[i]
        return pltpu.make_async_copy(src.at[rows(b)], raw.at[b, i], raw_l.at[b, i])

    def in_send(b, d):
        return remote(xs.at[b, rel[d]], rx.at[b, chip], in_s.at[b, d], in_r.at[b, d], rel[d] * 2 + core)

    def in_recv(b, d):
        return remote(xs.at[b, rel[d]], rx.at[b, rel[d]], in_s.at[b, d], in_r.at[b, d], rel[d] * 2 + core)

    def aux_send(b, d):
        return remote(auxs.at[b, rel[d]], axr.at[b, core, chip], ax_s.at[b, d], ax_r.at[b, d], rel[d] * 2 + core)

    def aux_recv(b, d):
        return remote(auxs.at[b, rel[d]], axr.at[b, core, rel[d]], ax_s.at[b, d], ax_r.at[b, d], rel[d] * 2 + core)

    def forward(b):
        return remote(rx.at[b, :, 0:2], rs.at[b], fw_s.at[b], fw_r.at[b], sib)

    def aux_forward(b):
        return remote(axr.at[b, core], axr.at[b, core], fa_s.at[b], fa_r.at[b], sib)

    def aux_forwarded(b):
        return remote(axr.at[b, core], axr.at[b, 1 - core], fa_s.at[b], fa_r.at[b], sib)

    def kv_send(b, d):
        return remote(okv.at[b, :, rel[d]], orx.at[b, 1:3, chip], kv_s.at[b, d], kv_r.at[b, d], rel[d] * 2 + core)

    def kv_recv(b, d):
        return remote(okv.at[b, :, rel[d]], orx.at[b, 1:3, rel[d]], kv_s.at[b, d], kv_r.at[b, d], rel[d] * 2 + core)

    def part_send(b):
        return remote(dqt.at[1, b], dqp.at[b], qp_s.at[b], qp_r.at[b], sib)

    def q_send(b, d):
        return remote(oq.at[b, rel[d]], orx.at[b, 0, chip], oq_s.at[b, d], oq_r.at[b, d], rel[d] * 2 + core)

    def q_recv(b, d):
        return remote(oq.at[b, rel[d]], orx.at[b, 0, rel[d]], oq_s.at[b, d], oq_r.at[b, d], rel[d] * 2 + core)

    barrier = pltpu.get_barrier_semaphore()
    peers = [r * 2 + core for r in rel] + [sib]
    for p in peers:
        pl.semaphore_signal(barrier, inc=1, device_id={'cp': p}, device_id_type=MESH)

    for i in range(5):
        raw_copy(i, nb - 1).start()
    lse_copy = pltpu.make_async_copy(lse_in, lsev, lse_l.at[0])
    lse_copy.start()

    eye = (lax.broadcasted_iota(jnp.int32, (ROWS, ROWS), 0)
           == lax.broadcasted_iota(jnp.int32, (ROWS, ROWS), 1))

    def relayout(b):
        for i in range(4):
            raw_copy(i, b).wait()
            xs[b, :, i] = jnp.swapaxes(raw[b, i], 0, 1)

    def dispatch(b):
        for d in (2, 0, 1):
            in_send(b, d).start()

    def stats(b):
        raw_copy(4, b).wait()
        oh = jnp.swapaxes(raw[b, 4], 0, 1)
        lse = lsev[:, rows(b)] * LOG2E
        for h in range(4):
            g = _dot(xs[b, h, 1], oh[h], 1, 1)
            auxs[b, h, 0] = lse[h:h + 1]
            auxs[b, h, 1] = jnp.sum(jnp.where(eye, g, 0.0), axis=0, keepdims=True)
        for d in (2, 0, 1):
            aux_send(b, d).start()
        rx[b, chip] = xs[b, chip]
        axr[b, core, chip] = auxs[b, chip]

    def load(n, c):
        for i in range(5):
            raw_copy(i, nb - 1 - n).start()
        return c

    relayout(nb - 1)
    pl.semaphore_wait(barrier, 4)
    dispatch(nb - 1)
    lax.fori_loop(1, nb, load, 0)
    lse_copy.wait()
    stats(nb - 1)

    def issue(n, c):
        b = nb - 1 - n
        relayout(b)
        dispatch(b)
        stats(b)
        return c

    lax.fori_loop(1, nb, issue, 0)

    kidx = lax.broadcasted_iota(jnp.int32, (tile, 1), 0)
    qidx = lax.broadcasted_iota(jnp.int32, (1, tile), 1)
    kpos = (kidx % ROWS) * 8 + (kidx // ROWS) * 2 + core

    def pair(b, qb, other, diag, fresh=False):
        if other:
            q = rs[qb, :, 0].reshape(tile, hd)
            do = rs[qb, :, 1].reshape(tile, hd)
            par = 1 - core
        else:
            q = rx[qb, :, 0].reshape(tile, hd)
            do = rx[qb, :, 1].reshape(tile, hd)
            par = core
        k = rx[b, :, 2].reshape(tile, hd)
        v = rx[b, :, 3].reshape(tile, hd)
        lse = jnp.concatenate([axr[qb, par, i, 0] for i in range(4)], axis=1)
        dd = jnp.concatenate([axr[qb, par, i, 1] for i in range(4)], axis=1)
        s = _dot(k, q, 1, 1)
        p = jnp.exp2(s * (scale * LOG2E) - lse)
        if diag:
            qpos = (qidx % ROWS) * 8 + (qidx // ROWS) * 2 + par
            p = jnp.where(kpos <= qpos, p, 0.0)
        dp = _dot(v, do, 1, 1)
        ds = (p * (dp - dd)).astype(BF16)
        gv = _dot(p.astype(BF16), do, 1, 0)
        gk = _dot(ds, q, 1, 0)
        gq = _dot(kt[...], ds, 1, 0)
        if fresh:
            dv[...] = gv
            dk[...] = gk
        else:
            dv[...] += gv
            dk[...] += gk
        if diag:
            dqt[int(other), qb] = gq
        else:
            dqt[int(other), qb] += gq

    def arrive(b):
        for d in range(3):
            in_recv(b, d).wait_recv()
            aux_recv(b, d).wait_recv()
        forward(b).start()
        aux_forward(b).start()

    def both(b, qb, diag):
        pair(b, qb, False, diag, fresh=diag)
        pair(b, qb, True, diag)

    def begin(b):
        kt[...] = rx[b, :, 2].reshape(tile, hd).astype(F32).T.astype(BF16)
        forward(b).wait_recv()
        aux_forwarded(b).wait_recv()

    def emit_kv(b):
        okv[b, 0] = (dk[...] * scale).astype(BF16).reshape(4, ROWS, hd)
        okv[b, 1] = dv[...].astype(BF16).reshape(4, ROWS, hd)
        for d in (2, 0, 1):
            kv_send(b, d).start()
        orx[b, 1:3, chip] = okv[b, :, chip]

    def step(n, c):
        b = nb - 1 - n
        begin(b)
        both(b, b, True)

        @pl.when(n == 0)
        def _():
            arrive(b - 1)

        def off(i, c):
            @pl.when(i == nb - 1)
            def _():
                arrive(b - 1)

            both(b, i, False)
            return c

        lax.fori_loop(b + 1, nb, off, 0)
        emit_kv(b)
        return c

    arrive(nb - 1)
    lax.fori_loop(0, nb - 1, step, 0)

    def finish(i):
        part_send(i).wait_recv()
        g = (dqt[0, i] + dqp[i]) * scale
        oq[i] = g.T.astype(BF16).reshape(4, ROWS, hd)
        for d in (2, 0, 1):
            q_send(i, d).start()
        orx[i, 0, chip] = oq[i, chip]

    begin(0)
    dv[...] = jnp.zeros_like(dv)
    dk[...] = jnp.zeros_like(dk)

    def last(n, c):
        i = nb - 1 - n
        both(0, i, False)
        part_send(i).start()

        @pl.when(n > 0)
        def _():
            finish(i + 1)

        return c

    lax.fori_loop(0, nb - 1, last, 0)
    pair(0, 0, True, True)
    part_send(0).start()
    pair(0, 0, False, True)
    emit_kv(0)
    finish(1)
    finish(0)

    def put(a, b):
        (dq_out, dk_out, dv_out)[a][rows(b)] = jnp.swapaxes(orx[b, a], 0, 1)

    def out_kv(b):
        for d in range(3):
            kv_recv(b, d).wait_recv()
        put(1, b)
        put(2, b)

    def out_q(b):
        for d in range(3):
            q_recv(b, d).wait_recv()
        put(0, b)

    def drain_kv(n, c):
        out_kv(nb - 1 - n)
        return c

    def drain_q(n, c):
        out_q(nb - 1 - n)
        return c

    lax.fori_loop(0, nb - 1, drain_kv, 0)
    lax.fori_loop(0, nb - 1, drain_q, 0)
    out_kv(0)
    out_q(0)

    def drain(b, c):
        for d in range(3):
            in_send(b, d).wait_send()
            aux_send(b, d).wait_send()
            kv_send(b, d).wait_send()
            q_send(b, d).wait_send()
        forward(b).wait_send()
        aux_forward(b).wait_send()
        part_send(b).wait_send()
        return c

    lax.fori_loop(0, nb, drain, 0)


def _store(a, b, c, x, y, z, sem):
    copies = [pltpu.make_async_copy(s, t, sem.at[i]) for i, (s, t) in enumerate(((a, x), (b, y), (c, z)))]
    for copy in copies:
        copy.start()
    for copy in copies:
        copy.wait()


def solution(mesh):
    rows = P(('data', 'cp'))
    cols = P(None, ('data', 'cp'))

    def local(q, k, v, o, dout, lse):
        c, h, d = q.shape
        nb = c // ROWS
        vm, dma = pltpu.VMEM, pltpu.SemaphoreType.DMA
        hbm = pl.BlockSpec(memory_space=pl.ANY)
        grads = pl.pallas_call(
            functools.partial(_kernel, nb),
            out_shape=[jax.ShapeDtypeStruct((c, h, d), BF16)] * 3,
            in_specs=[hbm] * 6,
            out_specs=[pl.BlockSpec(memory_space=pltpu.VMEM)] * 3,
            scratch_shapes=[
                vm((nb, 5, ROWS, h, d), BF16),
                vm((h, c), F32),
                vm((nb, h, 4, ROWS, d), BF16),
                vm((nb, h, 2, 1, ROWS), F32),
                vm((nb, 4, 4, ROWS, d), BF16),
                vm((nb, 4, 2, ROWS, d), BF16),
                vm((nb, 2, 4, 2, 1, ROWS), F32),
                vm((d, 4 * ROWS), BF16),
                vm((4 * ROWS, d), F32),
                vm((4 * ROWS, d), F32),
                vm((2, nb, d, 4 * ROWS), F32),
                vm((nb, d, 4 * ROWS), F32),
                vm((nb, 2, 4, ROWS, d), BF16),
                vm((nb, 4, ROWS, d), BF16),
                vm((nb, 3, h, ROWS, d), BF16),
                dma((nb, 5)), dma((1,)),
                dma((nb, 3)), dma((nb, 3)),
                dma((nb,)), dma((nb,)),
                dma((nb, 3)), dma((nb, 3)),
                dma((nb,)), dma((nb,)),
                dma((nb, 3)), dma((nb, 3)),
                dma((nb,)), dma((nb,)),
                dma((nb, 3)), dma((nb, 3)),
            ],
            compiler_params=pltpu.CompilerParams(
                collective_id=0, has_side_effects=True, vmem_limit_bytes=VMEM_LIMIT),
            name='attn_bwd',
        )(q, dout, k, v, o, lse)
        return pl.pallas_call(
            _store,
            out_shape=[jax.ShapeDtypeStruct((c, h, d), BF16)] * 3,
            in_specs=[pl.BlockSpec(memory_space=pltpu.VMEM)] * 3,
            out_specs=[hbm] * 3,
            scratch_shapes=[dma((3,))],
            compiler_params=pltpu.CompilerParams(vmem_limit_bytes=8 << 20),
            name='store',
        )(*grads)

    return jax.shard_map(local, mesh=mesh, in_specs=(rows, rows, rows, rows, rows, cols),
                         out_specs=(rows, rows, rows), check_vma=False)
```

```python
import functools
import math

import jax
import jax.numpy as jnp
from jax import lax
from jax.experimental import pallas as pl
from jax.experimental.pallas import tpu as pltpu
from jax.sharding import PartitionSpec as P

MESH = pl.DeviceIdType.MESH
F32 = jnp.float32
BF16 = jnp.bfloat16
ROWS = 128
VMEM_LIMIT = 50 << 20
LOG2E = math.log2(math.e)


def _dot(a, b, ca, cb):
    return lax.dot_general(a, b, (((ca,), (cb,)), ((), ())), preferred_element_type=F32)


def _kernel(nb, q_in, do_in, k_in, v_in, o_in, lse_in, dq_out, dk_out, dv_out,
            raw, lsev, xs, auxs, rx, rs, axr, kt, dk, dv, dqt, dqp, okv, oq, orx,
            raw_l, lse_l, in_s, in_r, fw_s, fw_r, ax_s, ax_r, fa_s, fa_r, kv_s, kv_r,
            qp_s, qp_r, oq_s, oq_r):
    hd = q_in.shape[-1]
    tile = 4 * ROWS
    scale = hd ** -0.5
    me = lax.axis_index('cp')
    core = me % 2
    chip = me // 2
    cx, cy = chip % 2, chip // 2
    sib = chip * 2 + (1 - core)
    rel = [cy * 2 + (1 - cx), (1 - cy) * 2 + cx, 3 - chip]

    def remote(src, dst, ss, rsem, dev):
        return pltpu.make_async_remote_copy(src_ref=src, dst_ref=dst, send_sem=ss, recv_sem=rsem,
                                            device_id={'cp': dev}, device_id_type=MESH)

    def rows(b):
        return pl.ds(pl.multiple_of(b * ROWS, ROWS), ROWS)

    def raw_copy(i, b):
        src = (q_in, do_in, k_in, v_in, o_in)[i]
        return pltpu.make_async_copy(src.at[rows(b)], raw.at[b, i], raw_l.at[b % 2])

    def landed(ref, sem):
        pltpu.make_async_copy(ref, ref, sem).wait()

    def in_send(b, d):
        return remote(xs.at[b, rel[d]], rx.at[b, chip], in_s.at[0], in_r.at[b], rel[d] * 2 + core)

    def aux_send(b, d):
        return remote(auxs.at[b, rel[d]], axr.at[b, core, chip], ax_s.at[0], ax_r.at[b], rel[d] * 2 + core)

    def forward(b):
        return remote(rx.at[b, :, 0:2], rs.at[b], fw_s.at[0], fw_r.at[b % 2], sib)

    def aux_forward(b):
        return remote(axr.at[b, core], axr.at[b, core], fa_s.at[0], fa_r.at[b % 2], sib)

    def aux_forwarded(b):
        return remote(axr.at[b, core], axr.at[b, 1 - core], fa_s.at[0], fa_r.at[b % 2], sib)

    def kv_send(b, d, g):
        return remote(okv.at[b, :, rel[d]], orx.at[b, 1:3, chip], kv_s.at[0], kv_r.at[g], rel[d] * 2 + core)

    def part_send(b):
        return remote(dqt.at[1, b], dqp.at[b], qp_s.at[0], qp_r.at[b], sib)

    def q_send(b, d, g):
        return remote(oq.at[b, rel[d]], orx.at[b, 0, chip], oq_s.at[0], oq_r.at[g], rel[d] * 2 + core)

    barrier = pltpu.get_barrier_semaphore()
    peers = [r * 2 + core for r in rel] + [sib]
    for p in peers:
        pl.semaphore_signal(barrier, inc=1, device_id={'cp': p}, device_id_type=MESH)

    def load(b):
        for i in range(5):
            raw_copy(i, b).start()

    load(nb - 1)
    load(nb - 2)
    lse_copy = pltpu.make_async_copy(lse_in, lsev, lse_l.at[0])
    lse_copy.start()

    eye = (lax.broadcasted_iota(jnp.int32, (ROWS, ROWS), 0)
           == lax.broadcasted_iota(jnp.int32, (ROWS, ROWS), 1))

    def relayout(b):
        landed(raw.at[b], raw_l.at[b % 2])
        for i in range(4):
            xs[b, :, i] = jnp.swapaxes(raw[b, i], 0, 1)

    def dispatch(b):
        for d in (2, 0, 1):
            in_send(b, d).start()

    def stats(b):
        oh = jnp.swapaxes(raw[b, 4], 0, 1)
        lse = lsev[:, rows(b)] * LOG2E
        for h in range(4):
            g = _dot(xs[b, h, 1], oh[h], 1, 1)
            auxs[b, h, 0] = lse[h:h + 1]
            auxs[b, h, 1] = jnp.sum(jnp.where(eye, g, 0.0), axis=0, keepdims=True)
        for d in (2, 0, 1):
            aux_send(b, d).start()
        rx[b, chip] = xs[b, chip]
        axr[b, core, chip] = auxs[b, chip]

    relayout(nb - 1)
    pl.semaphore_wait(barrier, 4)
    dispatch(nb - 1)
    load(nb - 3)
    lse_copy.wait()
    stats(nb - 1)

    def issue(n, c):
        b = nb - 1 - n
        relayout(b)
        dispatch(b)

        @pl.when(b >= 2)
        def _():
            load(b - 2)

        stats(b)
        return c

    lax.fori_loop(1, nb, issue, 0)

    kidx = lax.broadcasted_iota(jnp.int32, (tile, 1), 0)
    qidx = lax.broadcasted_iota(jnp.int32, (1, tile), 1)
    kpos = (kidx % ROWS) * 8 + (kidx // ROWS) * 2 + core

    def pair(b, qb, other, diag, fresh=False):
        if other:
            q = rs[qb, :, 0].reshape(tile, hd)
            do = rs[qb, :, 1].reshape(tile, hd)
            par = 1 - core
        else:
            q = rx[qb, :, 0].reshape(tile, hd)
            do = rx[qb, :, 1].reshape(tile, hd)
            par = core
        k = rx[b, :, 2].reshape(tile, hd)
        v = rx[b, :, 3].reshape(tile, hd)
        lse = jnp.concatenate([axr[qb, par, i, 0] for i in range(4)], axis=1)
        dd = jnp.concatenate([axr[qb, par, i, 1] for i in range(4)], axis=1)
        s = _dot(k, q, 1, 1)
        p = jnp.exp2(s * (scale * LOG2E) - lse)
        if diag:
            qpos = (qidx % ROWS) * 8 + (qidx // ROWS) * 2 + par
            p = jnp.where(kpos <= qpos, p, 0.0)
        dp = _dot(v, do, 1, 1)
        ds = (p * (dp - dd)).astype(BF16)
        gv = _dot(p.astype(BF16), do, 1, 0)
        gk = _dot(ds, q, 1, 0)
        gq = _dot(kt[...], ds, 1, 0)
        if fresh:
            dv[...] = gv
            dk[...] = gk
        else:
            dv[...] += gv
            dk[...] += gk
        if diag:
            dqt[int(other), qb] = gq
        else:
            dqt[int(other), qb] += gq

    def arrive(b):
        landed(rx.at[b, 0:3], in_r.at[b])
        landed(axr.at[b, 0, 0:3], ax_r.at[b])
        forward(b).start()
        aux_forward(b).start()

    def both(b, qb, diag):
        pair(b, qb, False, diag, fresh=diag)
        pair(b, qb, True, diag)

    def begin(b):
        kt[...] = rx[b, :, 2].reshape(tile, hd).astype(F32).T.astype(BF16)
        forward(b).wait_recv()
        aux_forwarded(b).wait_recv()

    def emit_kv(b, g):
        okv[b, 0] = (dk[...] * scale).astype(BF16).reshape(4, ROWS, hd)
        okv[b, 1] = dv[...].astype(BF16).reshape(4, ROWS, hd)
        for d in (2, 0, 1):
            kv_send(b, d, g).start()
        orx[b, 1:3, chip] = okv[b, :, chip]

    def step(n, c):
        b = nb - 1 - n
        begin(b)
        both(b, b, True)

        @pl.when(n == 0)
        def _():
            arrive(b - 1)

        def off(i, c):
            @pl.when(i == nb - 1)
            def _():
                arrive(b - 1)

            both(b, i, False)
            return c

        lax.fori_loop(b + 1, nb, off, 0)
        emit_kv(b, n // (nb - 2))
        return c

    arrive(nb - 1)
    lax.fori_loop(0, nb - 1, step, 0)

    def finish(i, g):
        part_send(i).wait_recv()
        total = (dqt[0, i] + dqp[i]) * scale
        oq[i] = total.T.astype(BF16).reshape(4, ROWS, hd)
        for d in (2, 0, 1):
            q_send(i, d, g).start()
        orx[i, 0, chip] = oq[i, chip]

    begin(0)
    dv[...] = jnp.zeros_like(dv)
    dk[...] = jnp.zeros_like(dk)

    def last(n, c):
        i = nb - 1 - n
        both(0, i, False)
        part_send(i).start()

        @pl.when(n > 0)
        def _():
            finish(i + 1, (nb - 2 - i) // 4)

        return c

    lax.fori_loop(0, nb - 1, last, 0)
    pair(0, 0, True, True)
    part_send(0).start()
    pair(0, 0, False, True)
    emit_kv(0, 2)
    finish(1, 2)
    finish(0, 3)

    def put(a, b):
        (dq_out, dk_out, dv_out)[a][rows(b)] = jnp.swapaxes(orx[b, a], 0, 1)

    def put_kv(b):
        put(1, b)
        put(2, b)

    def put_all(fn, lo, hi):
        def body(n, c):
            fn(hi - 1 - n)
            return c

        lax.fori_loop(0, hi - lo, body, 0)

    landed(orx.at[2:nb, 1:3, 0:3], kv_r.at[0])
    put_all(put_kv, 2, nb)
    landed(orx.at[1, 1:3, 0:3], kv_r.at[1])
    put_kv(1)
    landed(orx.at[4:nb, 0, 0:3], oq_r.at[0])
    put_all(functools.partial(put, 0), 4, nb)
    landed(orx.at[2:4, 0, 0:3], oq_r.at[1])
    put_all(functools.partial(put, 0), 2, 4)
    landed(orx.at[0, 1:3, 0:3], kv_r.at[2])
    put_kv(0)
    landed(orx.at[1, 0, 0:3], oq_r.at[2])
    put(0, 1)

    landed(xs.at[:, 0:3], in_s.at[0])
    landed(auxs.at[:, 0:3], ax_s.at[0])
    landed(rx.at[:, :, 0:2], fw_s.at[0])
    landed(axr.at[:, 0], fa_s.at[0])
    landed(dqt.at[1], qp_s.at[0])
    landed(okv.at[:, :, 0:3], kv_s.at[0])
    landed(orx.at[0, 0, 0:3], oq_r.at[3])
    put(0, 0)
    landed(oq.at[:, 0:3], oq_s.at[0])


def _store(a, b, c, x, y, z, sem):
    copies = [pltpu.make_async_copy(s, t, sem.at[i]) for i, (s, t) in enumerate(((a, x), (b, y), (c, z)))]
    for copy in copies:
        copy.start()
    for copy in copies:
        copy.wait()


def solution(mesh):
    rows = P(('data', 'cp'))
    cols = P(None, ('data', 'cp'))

    def local(q, k, v, o, dout, lse):
        c, h, d = q.shape
        nb = c // ROWS
        vm, dma = pltpu.VMEM, pltpu.SemaphoreType.DMA
        hbm = pl.BlockSpec(memory_space=pl.ANY)
        grads = pl.pallas_call(
            functools.partial(_kernel, nb),
            out_shape=[jax.ShapeDtypeStruct((c, h, d), BF16)] * 3,
            in_specs=[hbm] * 6,
            out_specs=[pl.BlockSpec(memory_space=pltpu.VMEM)] * 3,
            scratch_shapes=[
                vm((nb, 5, ROWS, h, d), BF16),
                vm((h, c), F32),
                vm((nb, h, 4, ROWS, d), BF16),
                vm((nb, h, 2, 1, ROWS), F32),
                vm((nb, 4, 4, ROWS, d), BF16),
                vm((nb, 4, 2, ROWS, d), BF16),
                vm((nb, 2, 4, 2, 1, ROWS), F32),
                vm((d, 4 * ROWS), BF16),
                vm((4 * ROWS, d), F32),
                vm((4 * ROWS, d), F32),
                vm((2, nb, d, 4 * ROWS), F32),
                vm((nb, d, 4 * ROWS), F32),
                vm((nb, 2, 4, ROWS, d), BF16),
                vm((nb, 4, ROWS, d), BF16),
                vm((nb, 3, h, ROWS, d), BF16),
                dma((2,)), dma((1,)),
                dma((1,)), dma((nb,)),
                dma((1,)), dma((2,)),
                dma((1,)), dma((nb,)),
                dma((1,)), dma((2,)),
                dma((1,)), dma((3,)),
                dma((1,)), dma((nb,)),
                dma((1,)), dma((4,)),
            ],
            compiler_params=pltpu.CompilerParams(
                collective_id=0, has_side_effects=True, vmem_limit_bytes=VMEM_LIMIT),
            name='attn_bwd',
        )(*(pltpu.with_memory_space_constraint(a, pltpu.HBM) for a in (q, dout, k, v, o, lse)))
        return pl.pallas_call(
            _store,
            out_shape=[jax.ShapeDtypeStruct((c, h, d), BF16)] * 3,
            in_specs=[pl.BlockSpec(memory_space=pltpu.VMEM)] * 3,
            out_specs=[hbm] * 3,
            scratch_shapes=[dma((3,))],
            compiler_params=pltpu.CompilerParams(vmem_limit_bytes=8 << 20),
            name='store',
        )(*grads)

    return jax.shard_map(local, mesh=mesh, in_specs=(rows, rows, rows, rows, rows, cols),
                         out_specs=(rows, rows, rows), check_vma=False)
```

```python
import functools
import math

import jax
import jax.numpy as jnp
from jax import lax
from jax.experimental import pallas as pl
from jax.experimental.pallas import tpu as pltpu
from jax.sharding import PartitionSpec as P

MESH = pl.DeviceIdType.MESH
F32 = jnp.float32
BF16 = jnp.bfloat16
ROWS = 128
VMEM_LIMIT = 50 << 20
LOG2E = math.log2(math.e)


def _dot(a, b, ca, cb):
    return lax.dot_general(a, b, (((ca,), (cb,)), ((), ())), preferred_element_type=F32)


def _kernel(nb, q_in, do_in, k_in, v_in, o_in, lse_in, dq_out, dk_out, dv_out,
            raw, lsev, xs, auxs, rx, rs, axr, kt, dk, dv, dqt, dqp, okv, oq, orx,
            raw_l, first_l, lse_l, in_s, in_r, fw_s, fw_r, ax_s, ax_r, fa_s, fa_r, kv_s, kv_r,
            qp_s, qp_r, oq_s, oq_r):
    hd = q_in.shape[-1]
    tile = 4 * ROWS
    scale = hd ** -0.5
    me = lax.axis_index('cp')
    core = me % 2
    chip = me // 2
    cx, cy = chip % 2, chip // 2
    sib = chip * 2 + (1 - core)
    rel = [cy * 2 + (1 - cx), (1 - cy) * 2 + cx, 3 - chip]

    def remote(src, dst, ss, rsem, dev):
        return pltpu.make_async_remote_copy(src_ref=src, dst_ref=dst, send_sem=ss, recv_sem=rsem,
                                            device_id={'cp': dev}, device_id_type=MESH)

    def rows(b):
        return pl.ds(pl.multiple_of(b * ROWS, ROWS), ROWS)

    def raw_copy(i, b, sem):
        src = (q_in, do_in, k_in, v_in, o_in)[i]
        return pltpu.make_async_copy(src.at[rows(b)], raw.at[b, i], sem)

    def landed(ref, sem):
        pltpu.make_async_copy(ref, ref, sem).wait()

    def in_send(b, d):
        return remote(xs.at[b, rel[d]], rx.at[b, chip], in_s.at[0], in_r.at[b], rel[d] * 2 + core)

    def in_piece(b, d, i):
        return remote(xs.at[b, rel[d], i], rx.at[b, chip, i], in_s.at[0], in_r.at[b], rel[d] * 2 + core)

    def aux_send(b, d):
        return remote(auxs.at[b, rel[d]], axr.at[b, core, chip], ax_s.at[0], ax_r.at[b], rel[d] * 2 + core)

    def forward(b):
        return remote(rx.at[b, :, 0:2], rs.at[b], fw_s.at[0], fw_r.at[b % 2], sib)

    def aux_forward(b):
        return remote(axr.at[b, core], axr.at[b, core], fa_s.at[0], fa_r.at[b % 2], sib)

    def aux_forwarded(b):
        return remote(axr.at[b, core], axr.at[b, 1 - core], fa_s.at[0], fa_r.at[b % 2], sib)

    def kv_send(b, d, g):
        return remote(okv.at[b, :, rel[d]], orx.at[b, 1:3, chip], kv_s.at[0], kv_r.at[g], rel[d] * 2 + core)

    def part_send(b):
        return remote(dqt.at[1, b], dqp.at[b], qp_s.at[0], qp_r.at[b], sib)

    def q_send(b, d, g):
        return remote(oq.at[b, rel[d]], orx.at[b, 0, chip], oq_s.at[0], oq_r.at[g], rel[d] * 2 + core)

    barrier = pltpu.get_barrier_semaphore()
    peers = [r * 2 + core for r in rel] + [sib]
    for p in peers:
        pl.semaphore_signal(barrier, inc=1, device_id={'cp': p}, device_id_type=MESH)

    def load(b):
        for i in range(5):
            raw_copy(i, b, raw_l.at[b % 2]).start()

    for i in range(5):
        raw_copy(i, nb - 1, first_l.at[i]).start()
    lse_copy = pltpu.make_async_copy(lse_in, lsev, lse_l.at[0])
    lse_copy.start()

    eye = (lax.broadcasted_iota(jnp.int32, (ROWS, ROWS), 0)
           == lax.broadcasted_iota(jnp.int32, (ROWS, ROWS), 1))

    def relayout(b):
        landed(raw.at[b], raw_l.at[b % 2])
        for i in range(4):
            xs[b, :, i] = jnp.swapaxes(raw[b, i], 0, 1)

    def dispatch(b):
        for d in (2, 0, 1):
            in_send(b, d).start()

    def stats(b):
        oh = jnp.swapaxes(raw[b, 4], 0, 1)
        lse = lsev[:, rows(b)] * LOG2E
        for h in range(4):
            g = _dot(xs[b, h, 1], oh[h], 1, 1)
            auxs[b, h, 0] = lse[h:h + 1]
            auxs[b, h, 1] = jnp.sum(jnp.where(eye, g, 0.0), axis=0, keepdims=True)
        for d in (2, 0, 1):
            aux_send(b, d).start()
        rx[b, chip] = xs[b, chip]
        axr[b, core, chip] = auxs[b, chip]

    last_block = nb - 1
    for i in range(4):
        raw_copy(i, last_block, first_l.at[i]).wait()
        xs[last_block, :, i] = jnp.swapaxes(raw[last_block, i], 0, 1)
        if i == 0:
            pl.semaphore_wait(barrier, 4)
        for d in (2, 0, 1):
            in_piece(last_block, d, i).start()
    load(nb - 2)
    load(nb - 3)
    raw_copy(4, last_block, first_l.at[4]).wait()
    lse_copy.wait()
    stats(nb - 1)

    def issue(n, c):
        b = nb - 1 - n
        relayout(b)
        dispatch(b)

        @pl.when(b >= 2)
        def _():
            load(b - 2)

        stats(b)
        return c

    lax.fori_loop(1, nb, issue, 0)

    kidx = lax.broadcasted_iota(jnp.int32, (tile, 1), 0)
    qidx = lax.broadcasted_iota(jnp.int32, (1, tile), 1)
    kpos = (kidx % ROWS) * 8 + (kidx // ROWS) * 2 + core

    def pair(b, qb, other, diag, fresh=False):
        if other:
            q = rs[qb, :, 0].reshape(tile, hd)
            do = rs[qb, :, 1].reshape(tile, hd)
            par = 1 - core
        else:
            q = rx[qb, :, 0].reshape(tile, hd)
            do = rx[qb, :, 1].reshape(tile, hd)
            par = core
        k = rx[b, :, 2].reshape(tile, hd)
        v = rx[b, :, 3].reshape(tile, hd)
        lse = jnp.concatenate([axr[qb, par, i, 0] for i in range(4)], axis=1)
        dd = jnp.concatenate([axr[qb, par, i, 1] for i in range(4)], axis=1)
        s = _dot(k, q, 1, 1)
        p = jnp.exp2(s * (scale * LOG2E) - lse)
        if diag:
            qpos = (qidx % ROWS) * 8 + (qidx // ROWS) * 2 + par
            p = jnp.where(kpos <= qpos, p, 0.0)
        dp = _dot(v, do, 1, 1)
        ds = (p * (dp - dd)).astype(BF16)
        gv = _dot(p.astype(BF16), do, 1, 0)
        gk = _dot(ds, q, 1, 0)
        gq = _dot(kt[...], ds, 1, 0)
        if fresh:
            dv[...] = gv
            dk[...] = gk
        else:
            dv[...] += gv
            dk[...] += gk
        if diag:
            dqt[int(other), qb] = gq
        else:
            dqt[int(other), qb] += gq

    def arrive(b):
        landed(rx.at[b, 0:3], in_r.at[b])
        landed(axr.at[b, 0, 0:3], ax_r.at[b])
        forward(b).start()
        aux_forward(b).start()

    def both(b, qb, diag):
        pair(b, qb, False, diag, fresh=diag)
        pair(b, qb, True, diag)

    def begin(b):
        kt[...] = rx[b, :, 2].reshape(tile, hd).astype(F32).T.astype(BF16)
        forward(b).wait_recv()
        aux_forwarded(b).wait_recv()

    def emit_kv(b, g):
        okv[b, 0] = (dk[...] * scale).astype(BF16).reshape(4, ROWS, hd)
        okv[b, 1] = dv[...].astype(BF16).reshape(4, ROWS, hd)
        for d in (2, 0, 1):
            kv_send(b, d, g).start()
        orx[b, 1:3, chip] = okv[b, :, chip]

    def step(n, c):
        b = nb - 1 - n
        begin(b)
        both(b, b, True)

        @pl.when(n == 0)
        def _():
            arrive(b - 1)

        def off(i, c):
            @pl.when(i == nb - 1)
            def _():
                arrive(b - 1)

            both(b, i, False)
            return c

        lax.fori_loop(b + 1, nb, off, 0)
        emit_kv(b, n // (nb - 2))
        return c

    arrive(nb - 1)
    lax.fori_loop(0, nb - 1, step, 0)

    def finish(i, g):
        part_send(i).wait_recv()
        total = (dqt[0, i] + dqp[i]) * scale
        oq[i] = total.T.astype(BF16).reshape(4, ROWS, hd)
        for d in (2, 0, 1):
            q_send(i, d, g).start()
        orx[i, 0, chip] = oq[i, chip]

    begin(0)
    dv[...] = jnp.zeros_like(dv)
    dk[...] = jnp.zeros_like(dk)

    def last(n, c):
        i = nb - 1 - n
        both(0, i, False)
        part_send(i).start()

        @pl.when(n > 0)
        def _():
            finish(i + 1, (nb - 2 - i) // 4)

        return c

    lax.fori_loop(0, nb - 1, last, 0)
    pair(0, 0, True, True)
    part_send(0).start()
    pair(0, 0, False, True)
    emit_kv(0, 2)
    finish(1, 2)
    finish(0, 3)

    def put(a, b):
        (dq_out, dk_out, dv_out)[a][rows(b)] = jnp.swapaxes(orx[b, a], 0, 1)

    def put_kv(b):
        put(1, b)
        put(2, b)

    def put_all(fn, lo, hi):
        def body(n, c):
            fn(hi - 1 - n)
            return c

        lax.fori_loop(0, hi - lo, body, 0)

    landed(orx.at[2:nb, 1:3, 0:3], kv_r.at[0])
    put_all(put_kv, 2, nb)
    landed(orx.at[1, 1:3, 0:3], kv_r.at[1])
    put_kv(1)
    landed(orx.at[4:nb, 0, 0:3], oq_r.at[0])
    put_all(functools.partial(put, 0), 4, nb)
    landed(orx.at[2:4, 0, 0:3], oq_r.at[1])
    put_all(functools.partial(put, 0), 2, 4)
    landed(orx.at[0, 1:3, 0:3], kv_r.at[2])
    put_kv(0)
    landed(orx.at[1, 0, 0:3], oq_r.at[2])
    put(0, 1)

    landed(xs.at[:, 0:3], in_s.at[0])
    landed(auxs.at[:, 0:3], ax_s.at[0])
    landed(rx.at[:, :, 0:2], fw_s.at[0])
    landed(axr.at[:, 0], fa_s.at[0])
    landed(dqt.at[1], qp_s.at[0])
    landed(okv.at[:, :, 0:3], kv_s.at[0])
    landed(orx.at[0, 0, 0:3], oq_r.at[3])
    put(0, 0)
    landed(oq.at[:, 0:3], oq_s.at[0])


def _store(a, b, c, x, y, z, sem):
    copies = [pltpu.make_async_copy(s, t, sem.at[i]) for i, (s, t) in enumerate(((a, x), (b, y), (c, z)))]
    for copy in copies:
        copy.start()
    for copy in copies:
        copy.wait()


def solution(mesh):
    rows = P(('data', 'cp'))
    cols = P(None, ('data', 'cp'))

    def local(q, k, v, o, dout, lse):
        c, h, d = q.shape
        nb = c // ROWS
        vm, dma = pltpu.VMEM, pltpu.SemaphoreType.DMA
        hbm = pl.BlockSpec(memory_space=pl.ANY)
        grads = pl.pallas_call(
            functools.partial(_kernel, nb),
            out_shape=[jax.ShapeDtypeStruct((c, h, d), BF16)] * 3,
            in_specs=[hbm] * 6,
            out_specs=[pl.BlockSpec(memory_space=pltpu.VMEM)] * 3,
            scratch_shapes=[
                vm((nb, 5, ROWS, h, d), BF16),
                vm((h, c), F32),
                vm((nb, h, 4, ROWS, d), BF16),
                vm((nb, h, 2, 1, ROWS), F32),
                vm((nb, 4, 4, ROWS, d), BF16),
                vm((nb, 4, 2, ROWS, d), BF16),
                vm((nb, 2, 4, 2, 1, ROWS), F32),
                vm((d, 4 * ROWS), BF16),
                vm((4 * ROWS, d), F32),
                vm((4 * ROWS, d), F32),
                vm((2, nb, d, 4 * ROWS), F32),
                vm((nb, d, 4 * ROWS), F32),
                vm((nb, 2, 4, ROWS, d), BF16),
                vm((nb, 4, ROWS, d), BF16),
                vm((nb, 3, h, ROWS, d), BF16),
                dma((2,)), dma((5,)), dma((1,)),
                dma((1,)), dma((nb,)),
                dma((1,)), dma((2,)),
                dma((1,)), dma((nb,)),
                dma((1,)), dma((2,)),
                dma((1,)), dma((3,)),
                dma((1,)), dma((nb,)),
                dma((1,)), dma((4,)),
            ],
            compiler_params=pltpu.CompilerParams(
                collective_id=0, has_side_effects=True, vmem_limit_bytes=VMEM_LIMIT),
            name='attn_bwd',
        )(*(pltpu.with_memory_space_constraint(a, pltpu.HBM) for a in (q, dout, k, v, o, lse)))
        return pl.pallas_call(
            _store,
            out_shape=[jax.ShapeDtypeStruct((c, h, d), BF16)] * 3,
            in_specs=[pl.BlockSpec(memory_space=pltpu.VMEM)] * 3,
            out_specs=[hbm] * 3,
            scratch_shapes=[dma((3,))],
            compiler_params=pltpu.CompilerParams(vmem_limit_bytes=8 << 20),
            name='store',
        )(*grads)

    return jax.shard_map(local, mesh=mesh, in_specs=(rows, rows, rows, rows, rows, cols),
                         out_specs=(rows, rows, rows), check_vma=False)
```

```python
import functools
import math

import jax
import jax.numpy as jnp
from jax import lax
from jax.experimental import pallas as pl
from jax.experimental.pallas import tpu as pltpu
from jax.sharding import PartitionSpec as P

MESH = pl.DeviceIdType.MESH
F32 = jnp.float32
BF16 = jnp.bfloat16
ROWS = 128
VMEM_LIMIT = 50 << 20
LOG2E = math.log2(math.e)


def _dot(a, b, ca, cb):
    return lax.dot_general(a, b, (((ca,), (cb,)), ((), ())), preferred_element_type=F32)


def _kernel(nb, q_in, do_in, k_in, v_in, o_in, lse_in, dq_out, dk_out, dv_out,
            raw, lsev, xs, auxs, rx, rs, axr, kt, dk, dv, dqt, dqp, okv, oq, orx,
            raw_l, first_l, lse_l, in_s, in_r, fw_s, fw_r, ax_s, ax_r, fa_s, fa_r, kv_s, kv_r,
            qp_s, qp_r, oq_s, oq_r, ready):
    hd = q_in.shape[-1]
    tile = 4 * ROWS
    scale = hd ** -0.5
    me = lax.axis_index('cp')
    core = me % 2
    chip = me // 2
    cx, cy = chip % 2, chip // 2
    sib = chip * 2 + (1 - core)
    rel = [cy * 2 + (1 - cx), (1 - cy) * 2 + cx, 3 - chip]

    def remote(src, dst, ss, rsem, dev):
        return pltpu.make_async_remote_copy(src_ref=src, dst_ref=dst, send_sem=ss, recv_sem=rsem,
                                            device_id={'cp': dev}, device_id_type=MESH)

    def rows(b):
        return pl.ds(pl.multiple_of(b * ROWS, ROWS), ROWS)

    def raw_copy(i, b, sem):
        src = (q_in, do_in, k_in, v_in, o_in)[i]
        return pltpu.make_async_copy(src.at[rows(b)], raw.at[b, i], sem)

    def landed(ref, sem):
        pltpu.make_async_copy(ref, ref, sem).wait()

    def in_send(b, d):
        return remote(xs.at[b, rel[d]], rx.at[b, chip], in_s.at[0], in_r.at[b], rel[d] * 2 + core)

    def in_piece(b, d, i):
        return remote(xs.at[b, rel[d], i], rx.at[b, chip, i], in_s.at[0], in_r.at[b], rel[d] * 2 + core)

    def aux_send(b, d):
        return remote(auxs.at[b, rel[d]], axr.at[b, core, chip], ax_s.at[0], ax_r.at[b], rel[d] * 2 + core)

    def forward(b):
        return remote(rx.at[b, :, 0:2], rs.at[b], fw_s.at[0], fw_r.at[b % 2], sib)

    def aux_forward(b):
        return remote(axr.at[b, core], axr.at[b, core], fa_s.at[0], fa_r.at[b % 2], sib)

    def aux_forwarded(b):
        return remote(axr.at[b, core], axr.at[b, 1 - core], fa_s.at[0], fa_r.at[b % 2], sib)

    def kv_send(b, d, g):
        return remote(okv.at[b, :, rel[d]], orx.at[b, 1:3, chip], kv_s.at[0], kv_r.at[g], rel[d] * 2 + core)

    def part_send(b):
        return remote(dqt.at[1, b], dqp.at[b], qp_s.at[0], qp_r.at[b], sib)

    def q_send(b, d, g):
        return remote(oq.at[b, rel[d]], orx.at[b, 0, chip], oq_s.at[0], oq_r.at[g], rel[d] * 2 + core)

    barrier = pltpu.get_barrier_semaphore()
    peers = [rel[0] * 2 + core, rel[1] * 2 + core, sib]
    for p in peers:
        pl.semaphore_signal(barrier, inc=1, device_id={'cp': p}, device_id_type=MESH)

    def load(b):
        for i in range(5):
            raw_copy(i, b, raw_l.at[b % 2]).start()

    for i in range(5):
        raw_copy(i, nb - 1, first_l.at[i]).start()
    lse_copy = pltpu.make_async_copy(lse_in, lsev, lse_l.at[0])
    lse_copy.start()

    eye = (lax.broadcasted_iota(jnp.int32, (ROWS, ROWS), 0)
           == lax.broadcasted_iota(jnp.int32, (ROWS, ROWS), 1))

    def relayout(b):
        landed(raw.at[b], raw_l.at[b % 2])
        for i in range(4):
            xs[b, :, i] = jnp.swapaxes(raw[b, i], 0, 1)

    def dispatch(b):
        for d in (2, 0, 1):
            in_send(b, d).start()

    def stats(b):
        oh = jnp.swapaxes(raw[b, 4], 0, 1)
        lse = lsev[:, rows(b)] * LOG2E
        for h in range(4):
            g = _dot(xs[b, h, 1], oh[h], 1, 1)
            auxs[b, h, 0] = lse[h:h + 1]
            auxs[b, h, 1] = jnp.sum(jnp.where(eye, g, 0.0), axis=0, keepdims=True)
        for d in (2, 0, 1):
            aux_send(b, d).start()
        rx[b, chip] = xs[b, chip]
        axr[b, core, chip] = auxs[b, chip]

    last_block = nb - 1
    for i in range(4):
        raw_copy(i, last_block, first_l.at[i]).wait()
        xs[last_block, :, i] = jnp.swapaxes(raw[last_block, i], 0, 1)
        if i == 0:
            pl.semaphore_wait(barrier, 3)
            pl.semaphore_signal(ready, inc=1, device_id={'cp': peers[0]}, device_id_type=MESH)
        for d in (0, 1):
            in_piece(last_block, d, i).start()
    load(nb - 2)
    load(nb - 3)
    relayout(nb - 2)
    for d in (0, 1):
        in_send(nb - 2, d).start()
    load(nb - 4)
    pl.semaphore_wait(ready, 1)
    in_send(nb - 1, 2).start()
    in_send(nb - 2, 2).start()
    raw_copy(4, nb - 1, first_l.at[4]).wait()
    lse_copy.wait()
    stats(nb - 1)
    stats(nb - 2)

    def issue(n, c):
        b = nb - 1 - n
        relayout(b)
        dispatch(b)

        @pl.when(b >= 2)
        def _():
            load(b - 2)

        stats(b)
        return c

    lax.fori_loop(2, nb, issue, 0)

    kidx = lax.broadcasted_iota(jnp.int32, (tile, 1), 0)
    qidx = lax.broadcasted_iota(jnp.int32, (1, tile), 1)
    kpos = (kidx % ROWS) * 8 + (kidx // ROWS) * 2 + core

    def pair(b, qb, other, diag, fresh=False):
        if other:
            q = rs[qb, :, 0].reshape(tile, hd)
            do = rs[qb, :, 1].reshape(tile, hd)
            par = 1 - core
        else:
            q = rx[qb, :, 0].reshape(tile, hd)
            do = rx[qb, :, 1].reshape(tile, hd)
            par = core
        k = rx[b, :, 2].reshape(tile, hd)
        v = rx[b, :, 3].reshape(tile, hd)
        lse = jnp.concatenate([axr[qb, par, i, 0] for i in range(4)], axis=1)
        dd = jnp.concatenate([axr[qb, par, i, 1] for i in range(4)], axis=1)
        s = _dot(k, q, 1, 1)
        p = jnp.exp2(s * (scale * LOG2E) - lse)
        if diag:
            qpos = (qidx % ROWS) * 8 + (qidx // ROWS) * 2 + par
            p = jnp.where(kpos <= qpos, p, 0.0)
        dp = _dot(v, do, 1, 1)
        ds = (p * (dp - dd)).astype(BF16)
        gv = _dot(p.astype(BF16), do, 1, 0)
        gk = _dot(ds, q, 1, 0)
        gq = _dot(kt[...], ds, 1, 0)
        if fresh:
            dv[...] = gv
            dk[...] = gk
        else:
            dv[...] += gv
            dk[...] += gk
        if diag:
            dqt[int(other), qb] = gq
        else:
            dqt[int(other), qb] += gq

    def arrive(b):
        landed(rx.at[b, 0:3], in_r.at[b])
        landed(axr.at[b, 0, 0:3], ax_r.at[b])
        forward(b).start()
        aux_forward(b).start()

    def both(b, qb, diag):
        pair(b, qb, False, diag, fresh=diag)
        pair(b, qb, True, diag)

    def begin(b):
        kt[...] = rx[b, :, 2].reshape(tile, hd).astype(F32).T.astype(BF16)
        forward(b).wait_recv()
        aux_forwarded(b).wait_recv()

    def emit_kv(b, g, order=(2, 0, 1)):
        okv[b, 0] = (dk[...] * scale).astype(BF16).reshape(4, ROWS, hd)
        okv[b, 1] = dv[...].astype(BF16).reshape(4, ROWS, hd)
        for d in order:
            kv_send(b, d, g).start()
        orx[b, 1:3, chip] = okv[b, :, chip]

    def step(n, c):
        b = nb - 1 - n
        begin(b)
        both(b, b, True)

        @pl.when(n == 0)
        def _():
            arrive(b - 1)

        def off(i, c):
            @pl.when(i == nb - 1)
            def _():
                arrive(b - 1)

            both(b, i, False)
            return c

        lax.fori_loop(b + 1, nb, off, 0)
        emit_kv(b, n // (nb - 2))
        return c

    arrive(nb - 1)
    lax.fori_loop(0, nb - 1, step, 0)

    def finish(i, g, order=(2, 0, 1)):
        part_send(i).wait_recv()
        total = (dqt[0, i] + dqp[i]) * scale
        oq[i] = total.T.astype(BF16).reshape(4, ROWS, hd)
        for d in order:
            q_send(i, d, g).start()
        orx[i, 0, chip] = oq[i, chip]

    begin(0)
    dv[...] = jnp.zeros_like(dv)
    dk[...] = jnp.zeros_like(dk)

    def last(n, c):
        i = nb - 1 - n
        both(0, i, False)
        part_send(i).start()

        @pl.when(n > 0)
        def _():
            finish(i + 1, (nb - 2 - i) // 4)

        return c

    lax.fori_loop(0, nb - 1, last, 0)
    pair(0, 0, True, True)
    part_send(0).start()
    pair(0, 0, False, True)
    emit_kv(0, 2, (2,))
    finish(1, 2, (2,))
    finish(0, 3, (2,))
    for d in (0, 1):
        kv_send(0, d, 2).start()
        q_send(1, d, 2).start()
        q_send(0, d, 3).start()

    def put(a, b):
        (dq_out, dk_out, dv_out)[a][rows(b)] = jnp.swapaxes(orx[b, a], 0, 1)

    def put_kv(b):
        put(1, b)
        put(2, b)

    def put_all(fn, lo, hi):
        def body(n, c):
            fn(hi - 1 - n)
            return c

        lax.fori_loop(0, hi - lo, body, 0)

    landed(orx.at[2:nb, 1:3, 0:3], kv_r.at[0])
    put_all(put_kv, 2, nb)
    landed(orx.at[1, 1:3, 0:3], kv_r.at[1])
    put_kv(1)
    landed(orx.at[4:nb, 0, 0:3], oq_r.at[0])
    put_all(functools.partial(put, 0), 4, nb)
    landed(orx.at[2:4, 0, 0:3], oq_r.at[1])
    put_all(functools.partial(put, 0), 2, 4)
    landed(orx.at[0, 1:3, 0:3], kv_r.at[2])
    put_kv(0)
    landed(orx.at[1, 0, 0:3], oq_r.at[2])
    put(0, 1)

    landed(xs.at[:, 0:3], in_s.at[0])
    landed(auxs.at[:, 0:3], ax_s.at[0])
    landed(rx.at[:, :, 0:2], fw_s.at[0])
    landed(axr.at[:, 0], fa_s.at[0])
    landed(dqt.at[1], qp_s.at[0])
    landed(okv.at[:, :, 0:3], kv_s.at[0])
    landed(orx.at[0, 0, 0:3], oq_r.at[3])
    put(0, 0)
    landed(oq.at[:, 0:3], oq_s.at[0])


def _store(a, b, c, x, y, z, sem):
    copies = [pltpu.make_async_copy(s, t, sem.at[i]) for i, (s, t) in enumerate(((a, x), (b, y), (c, z)))]
    for copy in copies:
        copy.start()
    for copy in copies:
        copy.wait()


def solution(mesh):
    rows = P(('data', 'cp'))
    cols = P(None, ('data', 'cp'))

    def local(q, k, v, o, dout, lse):
        c, h, d = q.shape
        nb = c // ROWS
        vm, dma = pltpu.VMEM, pltpu.SemaphoreType.DMA
        hbm = pl.BlockSpec(memory_space=pl.ANY)
        grads = pl.pallas_call(
            functools.partial(_kernel, nb),
            out_shape=[jax.ShapeDtypeStruct((c, h, d), BF16)] * 3,
            in_specs=[hbm] * 6,
            out_specs=[pl.BlockSpec(memory_space=pltpu.VMEM)] * 3,
            scratch_shapes=[
                vm((nb, 5, ROWS, h, d), BF16),
                vm((h, c), F32),
                vm((nb, h, 4, ROWS, d), BF16),
                vm((nb, h, 2, 1, ROWS), F32),
                vm((nb, 4, 4, ROWS, d), BF16),
                vm((nb, 4, 2, ROWS, d), BF16),
                vm((nb, 2, 4, 2, 1, ROWS), F32),
                vm((d, 4 * ROWS), BF16),
                vm((4 * ROWS, d), F32),
                vm((4 * ROWS, d), F32),
                vm((2, nb, d, 4 * ROWS), F32),
                vm((nb, d, 4 * ROWS), F32),
                vm((nb, 2, 4, ROWS, d), BF16),
                vm((nb, 4, ROWS, d), BF16),
                vm((nb, 3, h, ROWS, d), BF16),
                dma((2,)), dma((5,)), dma((1,)),
                dma((1,)), dma((nb,)),
                dma((1,)), dma((2,)),
                dma((1,)), dma((nb,)),
                dma((1,)), dma((2,)),
                dma((1,)), dma((3,)),
                dma((1,)), dma((nb,)),
                dma((1,)), dma((4,)),
                pltpu.SemaphoreType.REGULAR,
            ],
            compiler_params=pltpu.CompilerParams(
                collective_id=0, has_side_effects=True, vmem_limit_bytes=VMEM_LIMIT),
            name='attn_bwd',
        )(*(pltpu.with_memory_space_constraint(a, pltpu.HBM) for a in (q, dout, k, v, o, lse)))
        return pl.pallas_call(
            _store,
            out_shape=[jax.ShapeDtypeStruct((c, h, d), BF16)] * 3,
            in_specs=[pl.BlockSpec(memory_space=pltpu.VMEM)] * 3,
            out_specs=[hbm] * 3,
            scratch_shapes=[dma((3,))],
            compiler_params=pltpu.CompilerParams(vmem_limit_bytes=8 << 20),
            name='store',
        )(*grads)

    return jax.shard_map(local, mesh=mesh, in_specs=(rows, rows, rows, rows, rows, cols),
                         out_specs=(rows, rows, rows), check_vma=False)
```

```python
import functools
import math

import jax
import jax.numpy as jnp
from jax import lax
from jax.experimental import pallas as pl
from jax.experimental.pallas import tpu as pltpu
from jax.sharding import PartitionSpec as P

MESH = pl.DeviceIdType.MESH
F32 = jnp.float32
BF16 = jnp.bfloat16
ROWS = 128
VMEM_LIMIT = 50 << 20
LOG2E = math.log2(math.e)


def _dot(a, b, ca, cb):
    return lax.dot_general(a, b, (((ca,), (cb,)), ((), ())), preferred_element_type=F32)


def _kernel(nb, q_in, do_in, k_in, v_in, o_in, lse_in, dq_out, dk_out, dv_out,
            raw, lsev, xs, auxs, rx, rs, axr, kt, dk, dv, dqt, dqp, okv, oq, orx,
            raw_l, first_l, lse_l, in_s, in_r, fw_s, fw_r, ax_s, ax_r, fa_s, fa_r, kv_s, kv_r,
            qp_s, qp_r, oq_s, oq_r, ready):
    hd = q_in.shape[-1]
    tile = 4 * ROWS
    scale = hd ** -0.5
    me = lax.axis_index('cp')
    core = me % 2
    chip = me // 2
    cx, cy = chip % 2, chip // 2
    sib = chip * 2 + (1 - core)
    rel = [cy * 2 + (1 - cx), (1 - cy) * 2 + cx, 3 - chip]

    def remote(src, dst, ss, rsem, dev):
        return pltpu.make_async_remote_copy(src_ref=src, dst_ref=dst, send_sem=ss, recv_sem=rsem,
                                            device_id={'cp': dev}, device_id_type=MESH)

    def rows(b):
        return pl.ds(pl.multiple_of(b * ROWS, ROWS), ROWS)

    def raw_copy(i, b, sem):
        src = (q_in, do_in, k_in, v_in, o_in)[i]
        return pltpu.make_async_copy(src.at[rows(b)], raw.at[b, i], sem)

    def landed(ref, sem):
        pltpu.make_async_copy(ref, ref, sem).wait()

    def in_send(b, d):
        return remote(xs.at[b, rel[d]], rx.at[b, chip], in_s.at[0], in_r.at[b], rel[d] * 2 + core)

    def in_piece(b, d, i):
        return remote(xs.at[b, rel[d], i], rx.at[b, chip, i], in_s.at[0], in_r.at[b], rel[d] * 2 + core)

    def aux_send(b, d):
        return remote(auxs.at[b, rel[d]], axr.at[b, core, chip], ax_s.at[0], ax_r.at[b], rel[d] * 2 + core)

    def forward(b):
        return remote(rx.at[b, :, 0:2], rs.at[b], fw_s.at[0], fw_r.at[b % 2], sib)

    def aux_forward(b):
        return remote(axr.at[b, core], axr.at[b, core], fa_s.at[0], fa_r.at[b % 2], sib)

    def aux_forwarded(b):
        return remote(axr.at[b, core], axr.at[b, 1 - core], fa_s.at[0], fa_r.at[b % 2], sib)

    def kv_send(b, d, g):
        return remote(okv.at[b, :, rel[d]], orx.at[b, 1:3, chip], kv_s.at[0], kv_r.at[g], rel[d] * 2 + core)

    def part_send(b):
        return remote(dqt.at[1, b], dqp.at[b], qp_s.at[0], qp_r.at[b % 4], sib)

    def q_send(b, d, g):
        return remote(oq.at[b, rel[d]], orx.at[b, 0, chip], oq_s.at[0], oq_r.at[g], rel[d] * 2 + core)

    raw_copy(0, nb - 1, first_l.at[0]).start()
    barrier = pltpu.get_barrier_semaphore()
    peers = [rel[0] * 2 + core, rel[1] * 2 + core, sib]
    for p in peers:
        pl.semaphore_signal(barrier, inc=1, device_id={'cp': p}, device_id_type=MESH)

    def load(b):
        for i in range(5):
            raw_copy(i, b, raw_l.at[b % 2]).start()

    for i in range(1, 5):
        raw_copy(i, nb - 1, first_l.at[i]).start()
    lse_copy = pltpu.make_async_copy(lse_in, lsev, lse_l.at[0])
    lse_copy.start()

    eye = (lax.broadcasted_iota(jnp.int32, (ROWS, ROWS), 0)
           == lax.broadcasted_iota(jnp.int32, (ROWS, ROWS), 1))

    def relayout(b):
        landed(raw.at[b], raw_l.at[b % 2])
        for i in range(4):
            xs[b, :, i] = jnp.swapaxes(raw[b, i], 0, 1)

    def dispatch(b):
        for d in (2, 0, 1):
            in_send(b, d).start()

    def stats(b):
        oh = jnp.swapaxes(raw[b, 4], 0, 1)
        lse = lsev[:, rows(b)] * LOG2E
        for h in range(4):
            g = _dot(xs[b, h, 1], oh[h], 1, 1)
            auxs[b, h, 0] = lse[h:h + 1]
            auxs[b, h, 1] = jnp.sum(jnp.where(eye, g, 0.0), axis=0, keepdims=True)
        for d in (2, 0, 1):
            aux_send(b, d).start()
        rx[b, chip] = xs[b, chip]
        axr[b, core, chip] = auxs[b, chip]

    last_block = nb - 1
    for i in range(4):
        raw_copy(i, last_block, first_l.at[i]).wait()
        xs[last_block, :, i] = jnp.swapaxes(raw[last_block, i], 0, 1)
        if i == 0:
            pl.semaphore_wait(barrier, 3)
            pl.semaphore_signal(ready, inc=1, device_id={'cp': peers[0]}, device_id_type=MESH)
        for d in (0, 1):
            in_piece(last_block, d, i).start()
    load(nb - 2)
    load(nb - 3)
    relayout(nb - 2)
    for d in (0, 1):
        in_send(nb - 2, d).start()
    load(nb - 4)
    pl.semaphore_wait(ready, 1)
    in_send(nb - 1, 2).start()
    in_send(nb - 2, 2).start()
    raw_copy(4, nb - 1, first_l.at[4]).wait()
    lse_copy.wait()
    stats(nb - 1)
    stats(nb - 2)

    def issue(n, c):
        b = nb - 1 - n
        relayout(b)
        dispatch(b)

        @pl.when(b >= 2)
        def _():
            load(b - 2)

        stats(b)
        return c

    lax.fori_loop(2, nb, issue, 0)

    kidx = lax.broadcasted_iota(jnp.int32, (tile, 1), 0)
    qidx = lax.broadcasted_iota(jnp.int32, (1, tile), 1)
    kpos = (kidx % ROWS) * 8 + (kidx // ROWS) * 2 + core

    def pair(b, qb, other, diag, fresh=False):
        if other:
            q = rs[qb, :, 0].reshape(tile, hd)
            do = rs[qb, :, 1].reshape(tile, hd)
            par = 1 - core
        else:
            q = rx[qb, :, 0].reshape(tile, hd)
            do = rx[qb, :, 1].reshape(tile, hd)
            par = core
        k = rx[b, :, 2].reshape(tile, hd)
        v = rx[b, :, 3].reshape(tile, hd)
        lse = jnp.concatenate([axr[qb, par, i, 0] for i in range(4)], axis=1)
        dd = jnp.concatenate([axr[qb, par, i, 1] for i in range(4)], axis=1)
        s = _dot(k, q, 1, 1)
        p = jnp.exp2(s * (scale * LOG2E) - lse)
        if diag:
            qpos = (qidx % ROWS) * 8 + (qidx // ROWS) * 2 + par
            p = jnp.where(kpos <= qpos, p, 0.0)
        dp = _dot(v, do, 1, 1)
        ds = (p * (dp - dd)).astype(BF16)
        gv = _dot(p.astype(BF16), do, 1, 0)
        gk = _dot(ds, q, 1, 0)
        gq = _dot(kt[...], ds, 1, 0)
        if fresh:
            dv[...] = gv
            dk[...] = gk
        else:
            dv[...] += gv
            dk[...] += gk
        if diag:
            dqt[int(other), qb] = gq
        else:
            dqt[int(other), qb] += gq

    def arrive(b):
        landed(rx.at[b, 0:3], in_r.at[b])
        landed(axr.at[b, 0, 0:3], ax_r.at[b])
        forward(b).start()
        aux_forward(b).start()

    def both(b, qb, diag):
        pair(b, qb, False, diag, fresh=diag)
        pair(b, qb, True, diag)

    def begin(b):
        kt[...] = rx[b, :, 2].reshape(tile, hd).astype(F32).T.astype(BF16)
        forward(b).wait_recv()
        aux_forwarded(b).wait_recv()

    def emit_kv(b, g, order=(2, 0, 1)):
        okv[b, 0] = (dk[...] * scale).astype(BF16).reshape(4, ROWS, hd)
        okv[b, 1] = dv[...].astype(BF16).reshape(4, ROWS, hd)
        for d in order:
            kv_send(b, d, g).start()
        orx[b, 1:3, chip] = okv[b, :, chip]

    def step(n, c):
        b = nb - 1 - n
        begin(b)
        both(b, b, True)

        @pl.when(n == 0)
        def _():
            arrive(b - 1)

        def off(i, c):
            @pl.when(i == nb - 1)
            def _():
                arrive(b - 1)

            both(b, i, False)
            return c

        lax.fori_loop(b + 1, nb, off, 0)
        emit_kv(b, n // (nb - 2))
        return c

    arrive(nb - 1)
    lax.fori_loop(0, nb - 1, step, 0)

    def finish(i, g, order=(2, 0, 1)):
        part_send(i).wait_recv()
        total = (dqt[0, i] + dqp[i]) * scale
        oq[i] = total.T.astype(BF16).reshape(4, ROWS, hd)
        for d in order:
            q_send(i, d, g).start()
        orx[i, 0, chip] = oq[i, chip]

    begin(0)
    dv[...] = jnp.zeros_like(dv)
    dk[...] = jnp.zeros_like(dk)

    def last(n, c):
        i = nb - 1 - n
        both(0, i, False)
        part_send(i).start()

        @pl.when(n > 0)
        def _():
            finish(i + 1, (nb - 2 - i) // 4)

        return c

    lax.fori_loop(0, nb - 1, last, 0)
    pair(0, 0, True, True)
    part_send(0).start()
    pair(0, 0, False, True)
    emit_kv(0, 2, (2,))
    finish(1, 2, (2,))
    finish(0, 3, (2,))
    for d in (0, 1):
        kv_send(0, d, 2).start()
        q_send(1, d, 2).start()
        q_send(0, d, 3).start()

    def put(a, b):
        (dq_out, dk_out, dv_out)[a][rows(b)] = jnp.swapaxes(orx[b, a], 0, 1)

    def put_kv(b):
        put(1, b)
        put(2, b)

    def put_all(fn, lo, hi):
        def body(n, c):
            fn(hi - 1 - n)
            return c

        lax.fori_loop(0, hi - lo, body, 0)

    landed(orx.at[2:nb, 1:3, 0:3], kv_r.at[0])
    put_all(put_kv, 2, nb)
    landed(orx.at[1, 1:3, 0:3], kv_r.at[1])
    put_kv(1)
    landed(orx.at[4:nb, 0, 0:3], oq_r.at[0])
    put_all(functools.partial(put, 0), 4, nb)
    landed(orx.at[2:4, 0, 0:3], oq_r.at[1])
    put_all(functools.partial(put, 0), 2, 4)
    landed(orx.at[0, 1:3, 0:3], kv_r.at[2])
    put_kv(0)
    landed(orx.at[1, 0, 0:3], oq_r.at[2])
    put(0, 1)

    landed(xs.at[:, 0:3], in_s.at[0])
    landed(auxs.at[:, 0:3], ax_s.at[0])
    landed(rx.at[:, :, 0:2], fw_s.at[0])
    landed(axr.at[:, 0], fa_s.at[0])
    landed(dqt.at[1], qp_s.at[0])
    landed(okv.at[:, :, 0:3], kv_s.at[0])
    landed(orx.at[0, 0, 0:3], oq_r.at[3])
    put(0, 0)
    landed(oq.at[:, 0:3], oq_s.at[0])


def _store(a, b, c, x, y, z, sem):
    copies = [pltpu.make_async_copy(s, t, sem.at[i]) for i, (s, t) in enumerate(((a, x), (b, y), (c, z)))]
    for copy in copies:
        copy.start()
    for copy in copies:
        copy.wait()


def solution(mesh):
    rows = P(('data', 'cp'))
    cols = P(None, ('data', 'cp'))

    def local(q, k, v, o, dout, lse):
        c, h, d = q.shape
        nb = c // ROWS
        vm, dma = pltpu.VMEM, pltpu.SemaphoreType.DMA
        hbm = pl.BlockSpec(memory_space=pl.ANY)
        grads = pl.pallas_call(
            functools.partial(_kernel, nb),
            out_shape=[jax.ShapeDtypeStruct((c, h, d), BF16)] * 3,
            in_specs=[hbm] * 6,
            out_specs=[pl.BlockSpec(memory_space=pltpu.VMEM)] * 3,
            scratch_shapes=[
                vm((nb, 5, ROWS, h, d), BF16),
                vm((h, c), F32),
                vm((nb, h, 4, ROWS, d), BF16),
                vm((nb, h, 2, 1, ROWS), F32),
                vm((nb, 4, 4, ROWS, d), BF16),
                vm((nb, 4, 2, ROWS, d), BF16),
                vm((nb, 2, 4, 2, 1, ROWS), F32),
                vm((d, 4 * ROWS), BF16),
                vm((4 * ROWS, d), F32),
                vm((4 * ROWS, d), F32),
                vm((2, nb, d, 4 * ROWS), F32),
                vm((nb, d, 4 * ROWS), F32),
                vm((nb, 2, 4, ROWS, d), BF16),
                vm((nb, 4, ROWS, d), BF16),
                vm((nb, 3, h, ROWS, d), BF16),
                dma((2,)), dma((5,)), dma((1,)),
                dma((1,)), dma((nb,)),
                dma((1,)), dma((2,)),
                dma((1,)), dma((nb,)),
                dma((1,)), dma((2,)),
                dma((1,)), dma((3,)),
                dma((1,)), dma((4,)),
                dma((1,)), dma((4,)),
                pltpu.SemaphoreType.REGULAR,
            ],
            compiler_params=pltpu.CompilerParams(
                collective_id=0, has_side_effects=True, vmem_limit_bytes=VMEM_LIMIT),
            name='attn_bwd',
        )(*(pltpu.with_memory_space_constraint(a, pltpu.HBM) for a in (q, dout, k, v, o, lse)))
        return pl.pallas_call(
            _store,
            out_shape=[jax.ShapeDtypeStruct((c, h, d), BF16)] * 3,
            in_specs=[pl.BlockSpec(memory_space=pltpu.VMEM)] * 3,
            out_specs=[hbm] * 3,
            scratch_shapes=[dma((3,))],
            compiler_params=pltpu.CompilerParams(vmem_limit_bytes=8 << 20),
            name='store',
        )(*grads)

    return jax.shard_map(local, mesh=mesh, in_specs=(rows, rows, rows, rows, rows, cols),
                         out_specs=(rows, rows, rows), check_vma=False)
```
